32 devices in a mesh: section: 4 (over y, x), tp: 8 (over z, core).
Axes of the slice: x: 2, y: 2, z: 4, core: 2. Of those that a mesh axis runs over, the one named last changes fastest.
Arguments:
- awaiting_arrivals: bfloat16 [4, 8, 25, 1920], P('section', 'tp'), may hold values from -6 to 6
- label_numbers: int32 [5, 8], replicated, may hold values from 0 to 1000
- drawn_coarse_codes: int32 [1, 8, 30], replicated, may hold values from 0 to 4095
- discrete_prototypes: float32 [4096, 32], replicated, may hold values from -6 to 6
- code_raising_operator: bfloat16 [32, 1920], replicated, may hold values from -1 to 1
- placement_tier_features: bfloat16 [25, 1920], replicated, may hold values from -3 to 3
- label_feature_rows: bfloat16 [1001, 1920], P(None, 'tp'), may hold values from -6 to 6
- conditioned_gain_mapping: bfloat16 [4, 1920, 3, 1920], P('section', None, None, 'tp'), may hold values from -0.125 to 0.125
- conditioned_shift_addend: float32 [4, 3, 1920], P('section', None, 'tp'), may hold values from -3 to 3
- question_answer_operator: bfloat16 [4, 1920, 3, 1920], P('section', None, None, 'tp'), may hold values from -0.125 to 0.125
- mixing_return_operator: bfloat16 [4, 1920, 1920], P('section', None, 'tp'), may hold values from -0.125 to 0.125
- focus_sharpness_exponents: float32 [4, 30], P('section'), may hold values from 1 to 5.5
- prior_resolution_probes: bfloat16 [4, 2, 8, 30, 1920], P('section', None, 'tp'), may hold values from -0.75 to 0.75
- prior_resolution_answers: bfloat16 [4, 2, 8, 30, 1920], P('section', None, 'tp'), may hold values from -6 to 6
Outputs:
- section_out: bfloat16 [4, 2, 8, 25, 1920], P('section', None, 'tp')
The draws below stay inside these ranges and needn't reach their ends.
Inputs may be any that keep to these rules, and one draw needn't show every extreme that they name: `drawn_coarse_codes`: codebook indices of the maps of sides 1 to 4 of each image, one map after another, each row by row. `label_numbers`: class of each image; row r belongs to the micro-batch r - 4.
All inputs are finite; a program needn't handle non-finite values.
Results may differ from the reference program's by a relative error of at most 0.0151.
Values may be sent and summed in bfloat16 or wider, within the bound.
No kernel may reach another device: no remote copies, remote signals or barrier semaphores. Data moves between devices by JAX's collectives and lax.ppermute only.
A program may use at most 128 MiB of HBM per device.

```python
import jax
import jax.numpy as jnp
from jax import lax

HIDDEN_DIMENSION = 1920
FOCUS_GROUPS = 30
HEAD_DIM = 64
VOCAB = 4096
CVAE = 32
CLASSES = 1001
SIDE = 5
PATCHES_PER_GRID = 25
CTX_PREV = 30
PICTURES_PER_MB = 8
LAYERS_SECTION = 1
DEPTH_TOTAL = 4
NEW = 1
TICKS = 2
LABEL_ROWS = 5
N_SECTION = 4


def plant(drawn, stream_key, smallest, top_value):
    shape = drawn.shape
    index_at = [jax.random.randint(jax.random.fold_in(stream_key, axis), (), 0, shape[axis]) for axis in range(len(shape))]
    drawn = drawn.at[tuple(index_at)].set(smallest)
    longest = shape.index(max(shape))
    index_at[longest] = (index_at[longest] + 1) % shape[longest]
    return drawn.at[tuple(index_at)].set(top_value)


def shard_levels(stream_key, dims, split, smallest, high):
    loudness = 1.0
    for position, shards_of in split:
        heights = jax.random.uniform(jax.random.fold_in(jax.random.fold_in(stream_key, 6), position), (shards_of,), jnp.float32, smallest / len(split), high / len(split))
        loudness = loudness * jnp.repeat(jnp.exp(heights), dims[position] // shards_of).reshape((-1,) + (1,) * (len(dims) - 1 - position))
    return loudness


def gaussian(key, dims, scale, bound, cuts=(), held_as=jnp.bfloat16):
    level = shard_levels(key, dims, cuts, -0.22, 0.18) if cuts else 1.0
    values = jax.random.normal(key, dims, jnp.float32) * scale * level
    return jnp.minimum(jnp.maximum(values, -bound), bound).astype(held_as)


def setup_inputs(seed: int = 0) -> dict:
    seeds = jax.random.split(jax.random.key(seed), 15)
    return {
        "awaiting_arrivals": gaussian(seeds[0], (N_SECTION, PICTURES_PER_MB, PATCHES_PER_GRID, HIDDEN_DIMENSION), 1.0, 6.0, ((0, 4), (1, 8))),
        "label_numbers": plant(jax.random.randint(seeds[1], (LABEL_ROWS, PICTURES_PER_MB), 0, CLASSES), jax.random.fold_in(seeds[1], 1), 0, CLASSES - 1).astype(jnp.int32),
        "drawn_coarse_codes": plant(jax.random.randint(seeds[2], (NEW, PICTURES_PER_MB, CTX_PREV), 0, VOCAB), jax.random.fold_in(seeds[2], 1), 0, VOCAB - 1).astype(jnp.int32),
        "discrete_prototypes": gaussian(seeds[3], (VOCAB, CVAE), 1.0, 6.0, (), jnp.float32),
        "code_raising_operator": gaussian(seeds[4], (CVAE, HIDDEN_DIMENSION), CVAE ** -0.5, 1.0),
        "placement_tier_features": gaussian(seeds[5], (PATCHES_PER_GRID, HIDDEN_DIMENSION), 0.5, 3.0),
        "label_feature_rows": gaussian(seeds[6], (CLASSES, HIDDEN_DIMENSION), 1.0, 6.0, ((1, 8),)),
        "conditioned_gain_mapping": gaussian(seeds[7], (DEPTH_TOTAL, HIDDEN_DIMENSION, 3, HIDDEN_DIMENSION), HIDDEN_DIMENSION ** -0.5, 0.125, ((0, 4), (3, 8))),
        "conditioned_shift_addend": gaussian(seeds[8], (DEPTH_TOTAL, 3, HIDDEN_DIMENSION), 0.5, 3.0, ((0, 4), (2, 8)), jnp.float32),
        "question_answer_operator": gaussian(seeds[9], (DEPTH_TOTAL, HIDDEN_DIMENSION, 3, HIDDEN_DIMENSION), HIDDEN_DIMENSION ** -0.5, 0.125, ((0, 4), (3, 8))),
        "mixing_return_operator": gaussian(seeds[10], (DEPTH_TOTAL, HIDDEN_DIMENSION, HIDDEN_DIMENSION), HIDDEN_DIMENSION ** -0.5, 0.125, ((0, 4), (2, 8))),
        "focus_sharpness_exponents": jnp.clip(1.0 + 4.5 * jax.random.uniform(seeds[11], (DEPTH_TOTAL, FOCUS_GROUPS), jnp.float32) ** shard_levels(seeds[11], (DEPTH_TOTAL, FOCUS_GROUPS), ((0, 4),), -0.2, 0.2), 1.0, 5.5),
        "prior_resolution_probes": gaussian(seeds[12], (DEPTH_TOTAL, TICKS, PICTURES_PER_MB, CTX_PREV, HIDDEN_DIMENSION), 0.125, 0.75, ((0, 4), (2, 8))),
        "prior_resolution_answers": gaussian(seeds[13], (DEPTH_TOTAL, TICKS, PICTURES_PER_MB, CTX_PREV, HIDDEN_DIMENSION), 1.0, 6.0, ((0, 4), (2, 8))),
    }


LOG_CAP = 4.605170185988092

def crossing_matrix(target, coarse):
    fine_index = jnp.arange(target, dtype=jnp.float32)
    coarse_index = jnp.arange(coarse, dtype=jnp.float32)
    begins = jnp.maximum(fine_index[:, None] / target, coarse_index[None, :] / coarse)
    finish = jnp.minimum((fine_index[:, None] + 1.0) / target, (coarse_index[None, :] + 1.0) / coarse)
    return jnp.maximum(finish - begins, 0.0) * target

def resampler():
    blocks = []
    for coarse in range(1, SIDE):
        crossing = crossing_matrix(SIDE, coarse)
        blocks.append((crossing[:, None, :, None] * crossing[None, :, None, :]).reshape(SIDE * SIDE, coarse * coarse))
    return jnp.concatenate(blocks, axis=1)

def embed(drawn_coarse_codes, discrete_prototypes, code_raising_operator, placement_tier_features, resample_table):
    looked_up = discrete_prototypes[drawn_coarse_codes]
    mapped = jnp.einsum('tc,nicv->nitv', resample_table, looked_up, precision=lax.Precision.HIGHEST).astype(jnp.bfloat16)
    leading = mapped.shape[:3]
    projected_rows = jnp.dot(mapped.reshape(-1, mapped.shape[3]), code_raising_operator, preferred_element_type=jnp.float32)
    projected_rows = projected_rows.reshape(leading + (code_raising_operator.shape[1],))
    return (projected_rows + placement_tier_features.astype(jnp.float32)).astype(jnp.bfloat16)

def norm_mod(latent_stream, scale_term, offset_term):
    widened = latent_stream.astype(jnp.float32)
    average = lax.optimization_barrier(jnp.mean(widened, axis=-1, keepdims=True))
    centred = widened - average
    spread = lax.optimization_barrier(jnp.mean(centred * centred, axis=-1, keepdims=True))
    normed = centred * lax.rsqrt(spread + 1e-06) * (1.0 + scale_term[:, None, :]) + offset_term[:, None, :]
    return normed.astype(jnp.bfloat16)

def attention(qkv, log_scale, cached_keys, cached_values):
    images = qkv.shape[0]
    count = qkv.shape[1]
    widened = lax.optimization_barrier(qkv).astype(jnp.float32)
    query = widened[:, :, 0].reshape(images, count, FOCUS_GROUPS, HEAD_DIM)
    new_keys = widened[:, :, 1].reshape(images, count, FOCUS_GROUPS, HEAD_DIM)
    new_values = qkv[:, :, 2].reshape(images, count, FOCUS_GROUPS, HEAD_DIM)
    head_mult = jnp.exp(jnp.minimum(log_scale, LOG_CAP))
    query = query * lax.rsqrt(lax.optimization_barrier(jnp.sum(query * query, axis=-1, keepdims=True)) + 1e-06) * head_mult[:, None]
    new_keys = new_keys * lax.rsqrt(lax.optimization_barrier(jnp.sum(new_keys * new_keys, axis=-1, keepdims=True)) + 1e-06)
    all_keys = jnp.concatenate([cached_keys.astype(jnp.float32).reshape(images, -1, FOCUS_GROUPS, HEAD_DIM), new_keys], axis=1)
    all_values = jnp.concatenate([cached_values.reshape(images, -1, FOCUS_GROUPS, HEAD_DIM), new_values], axis=1)
    scores = jnp.einsum('iqhd,ikhd->ihqk', query, all_keys, precision=lax.Precision.HIGHEST)
    maximum = lax.optimization_barrier(jnp.max(scores, axis=-1, keepdims=True))
    weights = jnp.exp(scores - maximum)
    probabilities = (weights / lax.optimization_barrier(jnp.sum(weights, axis=-1, keepdims=True))).astype(jnp.bfloat16)
    mixed = jnp.einsum('ihqk,ikhd->iqhd', probabilities, all_values, preferred_element_type=jnp.float32)
    return mixed.reshape(images, count, FOCUS_GROUPS * HEAD_DIM).astype(jnp.bfloat16)

def block_params(latent_stream, gated_response, mod_matrix, mod_shift, qkv_matrix, out_matrix, log_scale, cached_keys, cached_values):
    images = latent_stream.shape[0]
    modulation = jnp.dot(gated_response, mod_matrix.reshape(HIDDEN_DIMENSION, 3 * HIDDEN_DIMENSION), preferred_element_type=jnp.float32)
    modulation = modulation.reshape(images, 3, HIDDEN_DIMENSION) + mod_shift
    normed = norm_mod(latent_stream, modulation[:, 1], modulation[:, 2])
    qkv = jnp.dot(normed.reshape(-1, HIDDEN_DIMENSION), qkv_matrix.reshape(HIDDEN_DIMENSION, 3 * HIDDEN_DIMENSION), preferred_element_type=jnp.float32)
    qkv = qkv.astype(jnp.bfloat16).reshape(images, PATCHES_PER_GRID, 3, HIDDEN_DIMENSION)
    attended = attention(qkv, log_scale, cached_keys, cached_values)
    projected = jnp.dot(attended.reshape(-1, HIDDEN_DIMENSION), out_matrix, preferred_element_type=jnp.float32)
    projected = lax.optimization_barrier(projected.astype(jnp.bfloat16)).astype(jnp.float32).reshape(images, PATCHES_PER_GRID, HIDDEN_DIMENSION)
    return (latent_stream.astype(jnp.float32) + modulation[:, 0][:, None, :] * projected).astype(jnp.bfloat16)

def reference(awaiting_arrivals, label_numbers, drawn_coarse_codes, discrete_prototypes, code_raising_operator, placement_tier_features, label_feature_rows, conditioned_gain_mapping, conditioned_shift_addend, question_answer_operator, mixing_return_operator, focus_sharpness_exponents, prior_resolution_probes, prior_resolution_answers):
    entering = embed(drawn_coarse_codes, discrete_prototypes, code_raising_operator, placement_tier_features, resampler())
    passed_along_activation = [awaiting_arrivals[segment_ordinal] for segment_ordinal in range(N_SECTION)]
    emitted = []
    for clock_tick in range(TICKS):
        produced = []
        for segment_ordinal in range(N_SECTION):
            class_rows = label_numbers[clock_tick - segment_ordinal - 1 + N_SECTION]
            gated_response = jax.nn.silu(label_feature_rows[class_rows].astype(jnp.float32)).astype(jnp.bfloat16)
            latent_stream = passed_along_activation[segment_ordinal]
            for inner_block in range(LAYERS_SECTION):
                depth_number = segment_ordinal * LAYERS_SECTION + inner_block
                latent_stream = block_params(latent_stream, gated_response, conditioned_gain_mapping[depth_number], conditioned_shift_addend[depth_number], question_answer_operator[depth_number], mixing_return_operator[depth_number], focus_sharpness_exponents[depth_number], prior_resolution_probes[depth_number, clock_tick], prior_resolution_answers[depth_number, clock_tick])
            produced.append(latent_stream)
        emitted.append(jnp.stack(produced))
        if clock_tick + 1 < TICKS:
            passed_along_activation = [entering[clock_tick]] + produced[:-1]
    return jnp.stack(emitted, axis=1)
```

```python
import jax
import jax.numpy as jnp
from jax import lax
from jax.experimental import pallas as pl
from jax.experimental.pallas import tpu as pltpu
from jax.sharding import PartitionSpec as P
import numpy as np

FOCUS_GROUPS = 30
HEAD_DIM = 64
SIDE = 5


LOG_CAP = 4.605170185988092


def shifted(value, axis, steps):
    count = lax.axis_size(axis)
    first, last = (max(0, -steps), min(count, count - steps))
    return lax.ppermute(value, axis, [(source, source + steps) for source in range(first, last)])


def crossing_matrix(target, coarse):
    fine_index = jnp.arange(target, dtype=jnp.float32)
    coarse_index = jnp.arange(coarse, dtype=jnp.float32)
    begins = jnp.maximum(fine_index[:, None] / target, coarse_index[None, :] / coarse)
    finish = jnp.minimum(
        (fine_index[:, None] + 1.0) / target, (coarse_index[None, :] + 1.0) / coarse
    )
    return jnp.maximum(finish - begins, 0.0) * target


def resampler():
    blocks = []
    for coarse in range(1, SIDE):
        crossing = crossing_matrix(SIDE, coarse)
        blocks.append(
            (crossing[:, None, :, None] * crossing[None, :, None, :]).reshape(
                SIDE * SIDE, coarse * coarse
            )
        )
    return jnp.concatenate(blocks, axis=1)


def embed(
    drawn_coarse_codes,
    discrete_prototypes,
    code_raising_operator,
    placement_tier_features,
    resample_table,
):
    looked_up = discrete_prototypes[drawn_coarse_codes]
    mapped = jnp.einsum(
        "tc,nicv->nitv", resample_table, looked_up, precision=lax.Precision.HIGHEST
    ).astype(jnp.bfloat16)
    leading = mapped.shape[:3]
    projected_rows = jnp.dot(
        mapped.reshape(-1, mapped.shape[3]),
        code_raising_operator,
        preferred_element_type=jnp.float32,
    )
    projected_rows = projected_rows.reshape(leading + (code_raising_operator.shape[1],))
    return (projected_rows + placement_tier_features.astype(jnp.float32)).astype(jnp.bfloat16)


def norm_mod(latent_stream, scale_term, offset_term):
    widened = latent_stream.astype(jnp.float32)
    average = jnp.mean(widened, axis=-1, keepdims=True)
    centred = widened - average
    spread = jnp.mean(centred * centred, axis=-1, keepdims=True)
    normed = (
        centred * lax.rsqrt(spread + 1e-06) * (1.0 + scale_term[:, None, :])
        + offset_term[:, None, :]
    )
    return normed.astype(jnp.bfloat16)


def attention(qkv_cols, log_scale, cached_keys, cached_values):
    qkv = lax.all_to_all(qkv_cols, "tp", split_axis=0, concat_axis=3, tiled=True)
    images = qkv.shape[0]
    count = qkv.shape[1]
    widened = qkv.astype(jnp.float32)
    query = widened[:, :, 0].reshape(images, count, FOCUS_GROUPS, HEAD_DIM)
    new_keys = widened[:, :, 1].reshape(images, count, FOCUS_GROUPS, HEAD_DIM)
    new_values = qkv[:, :, 2].reshape(images, count, FOCUS_GROUPS, HEAD_DIM)
    head_mult = jnp.exp(jnp.minimum(log_scale, LOG_CAP))
    query = (
        query
        * lax.rsqrt(jnp.sum(query * query, axis=-1, keepdims=True) + 1e-06)
        * head_mult[:, None]
    )
    new_keys = new_keys * lax.rsqrt(jnp.sum(new_keys * new_keys, axis=-1, keepdims=True) + 1e-06)
    all_keys = jnp.concatenate(
        [cached_keys.astype(jnp.float32).reshape(images, -1, FOCUS_GROUPS, HEAD_DIM), new_keys],
        axis=1,
    )
    all_values = jnp.concatenate(
        [cached_values.reshape(images, -1, FOCUS_GROUPS, HEAD_DIM), new_values], axis=1
    )
    scores = jnp.einsum("iqhd,ikhd->ihqk", query, all_keys, precision=lax.Precision.HIGHEST)
    maximum = jnp.max(scores, axis=-1, keepdims=True)
    weights = jnp.exp(scores - maximum)
    probabilities = (weights / jnp.sum(weights, axis=-1, keepdims=True)).astype(jnp.bfloat16)
    mixed = jnp.einsum(
        "ihqk,ikhd->iqhd", probabilities, all_values, preferred_element_type=jnp.float32
    )
    return mixed.reshape(images, count, FOCUS_GROUPS * HEAD_DIM).astype(jnp.bfloat16)


def project_out(attended, out_matrix):
    return jnp.dot(
        lax.all_gather(attended, "tp", axis=0, tiled=True),
        out_matrix,
        preferred_element_type=jnp.float32,
    )


def pass_on(latent_stream):
    return shifted(latent_stream, "section", 1)


def general(
    awaiting_arrivals,
    label_numbers,
    drawn_coarse_codes,
    discrete_prototypes,
    code_raising_operator,
    placement_tier_features,
    label_feature_rows,
    conditioned_gain_mapping,
    conditioned_shift_addend,
    question_answer_operator,
    mixing_return_operator,
    focus_sharpness_exponents,
    prior_resolution_probes,
    prior_resolution_answers,
):
    sections = lax.axis_size("section")
    section_at = lax.axis_index("section")
    group_index = lax.axis_index("tp")
    moments = prior_resolution_probes.shape[1]
    width = question_answer_operator.shape[1]
    column_width = question_answer_operator.shape[3]
    images = drawn_coarse_codes.shape[1]
    resident_pictures = awaiting_arrivals.shape[1]
    class_rows = lax.dynamic_slice_in_dim(label_numbers, sections - 1 - section_at, moments, 0)
    class_part = jnp.take(label_feature_rows, class_rows, axis=0)
    activated_part = jax.nn.silu(class_part.astype(jnp.float32)).astype(jnp.bfloat16)
    gated_response = lax.all_gather(activated_part, "tp", axis=2, tiled=True)
    flat_active = gated_response.reshape(moments * images, width)
    inner_block = 0
    local_mod = conditioned_gain_mapping[inner_block].reshape(width, 3 * column_width)
    modulated = jnp.dot(flat_active, local_mod, preferred_element_type=jnp.float32)
    mod_list = [
        modulated.reshape(moments, images, 3, column_width) + conditioned_shift_addend[inner_block]
    ]
    mod_cols = jnp.stack(mod_list)
    resample_table = resampler()
    emitted = []
    mod_rows = lax.all_to_all(mod_cols, "tp", split_axis=2, concat_axis=4, tiled=True)
    own_tokens = lax.dynamic_slice_in_dim(
        drawn_coarse_codes, group_index * resident_pictures, resident_pictures, 1
    )
    entering = embed(
        own_tokens,
        discrete_prototypes,
        code_raising_operator,
        placement_tier_features,
        resample_table,
    )
    passed_along_activation = awaiting_arrivals[0]
    for clock_tick in range(moments):
        latent_stream = passed_along_activation
        inner_block = 0
        modulation = mod_rows[inner_block, clock_tick]
        normed = norm_mod(latent_stream, modulation[:, 1], modulation[:, 2])
        local_qkv = question_answer_operator[inner_block].reshape(width, 3 * column_width)

        def body_product(portion, offset, local_qkv=local_qkv):
            return jnp.dot(portion, local_qkv, preferred_element_type=jnp.float32).astype(
                jnp.bfloat16
            )

        qkv_cols = body_product(lax.all_gather(normed, "tp", axis=0, tiled=True), jnp.int32(0))
        qkv_cols = qkv_cols.reshape(qkv_cols.shape[0], qkv_cols.shape[1], 3, column_width)
        attended = attention(
            qkv_cols,
            focus_sharpness_exponents[inner_block],
            prior_resolution_probes[inner_block, clock_tick],
            prior_resolution_answers[inner_block, clock_tick],
        )
        projected_cols = project_out(attended, mixing_return_operator[inner_block]).astype(
            jnp.bfloat16
        )
        projected = lax.all_to_all(projected_cols, "tp", split_axis=0, concat_axis=2, tiled=True)
        latent_stream = (
            latent_stream.astype(jnp.float32)
            + modulation[:, 0][:, None, :] * projected.astype(jnp.float32)
        ).astype(jnp.bfloat16)
        emitted.append(latent_stream)
        if clock_tick + 1 < moments:
            arrived = pass_on(latent_stream)
            passed_along_activation = jnp.where(section_at == 0, entering[clock_tick], arrived)
    result = jnp.stack(emitted)
    return result[None]


SLOT = 32
F32 = jnp.float32
BF16 = jnp.bfloat16


def first_head(pair, pair_width, head_dim):
    return (2 * pair * pair_width + head_dim) // (2 * head_dim)


class Plan:
    def __init__(self, section, tp, args):
        (arrivals, _, codes, prototypes, _, placement, labels, gain, _, _, _, sharp, probes, _) = args
        self.section, self.tp = section, tp
        self.pairs = tp // 2
        self.width = gain.shape[1]
        self.cols = gain.shape[3]
        self.pair_cols = 2 * self.cols
        self.heads = sharp.shape[1]
        self.head_dim = self.width // self.heads
        self.tokens = placement.shape[0]
        self.ctx = probes.shape[3]
        self.ticks = probes.shape[1]
        self.images = codes.shape[1]
        self.resident = arrivals.shape[1]
        self.lanes = self.pairs * SLOT
        self.classes = labels.shape[0]
        self.vocab, self.code_dim = prototypes.shape
        starts = [first_head(p, self.pair_cols, self.head_dim) for p in range(self.pairs + 1)]
        self.starts = starts
        self.counts = [starts[p + 1] - starts[p] for p in range(self.pairs)]
        self.most = max(self.counts)
        self.left = [p * self.pair_cols - starts[p] * self.head_dim for p in range(self.pairs)]
        self.need = [
            max(0, starts[p + 1] * self.head_dim - (p + 1) * self.pair_cols)
            for p in range(self.pairs)
        ]
        self.halo = max(self.need)
        self.rows = max(self.pair_cols + self.halo, self.most * self.head_dim - min(self.left))
        self.fits = (
            tp % 2 == 0
            and self.pairs & (self.pairs - 1) == 0
            and gain.shape[0] == 1
            and codes.shape[0] == 1
            and self.ticks == 2
            and self.resident == 1
            and self.images == tp
            and self.cols % 16 == 0
            and self.head_dim == HEAD_DIM
            and starts[-1] == self.heads
            and max(self.left) <= 0
            and all(offset % 16 == 0 for offset in self.left)
            and 0 < self.halo <= self.cols
            and self.halo % 16 == 0
            and self.tokens <= SLOT
            and self.ctx <= SLOT
            and self.lanes == 128
        )


def whole(shape=None, space=pltpu.VMEM):
    return pl.BlockSpec(memory_space=space)


def dot(left, right, contract=((1,), (0,)), precision=None):
    return lax.dot_general(
        left, right, (contract, ((), ())), preferred_element_type=F32, precision=precision
    )


def spread(rows, tick, plan):
    total = rows.shape[0]
    row = lax.broadcasted_iota(jnp.int32, (total, plan.lanes), 0)
    lane = lax.broadcasted_iota(jnp.int32, (total, plan.lanes), 1)
    pick = (row == tick * plan.pairs + lane // SLOT).astype(F32)
    return dot(rows, pick, ((0,), (0,)), lax.Precision.HIGHEST)


def label_kernel(plan, labels, table, out, picked):
    section_at = lax.axis_index("section")
    place = lax.broadcasted_iota(jnp.int32, (1, plan.classes), 1)
    row = 0
    for core in range(2):
        for tick in range(plan.ticks):
            for pair in range(plan.pairs):
                label = labels[tick - section_at + plan.section - 1, 2 * pair + core]
                picked[row : row + 1, :] = (place == label).astype(F32)
                row += 1
    value = dot(picked[...].astype(BF16), table[...], ((1,), (1,)))
    out[...] = (value / (1.0 + jnp.exp(-value))).astype(BF16)


def modulation_kernel(plan, *refs):
    pieces = refs[: plan.pairs]
    matrix, addend, mine, other, active = refs[plan.pairs :]
    place = lax.axis_index("tp")
    core, pair = place % 2, place // 2
    step = pl.program_id(0)
    rows = plan.ticks * plan.images

    @pl.when(step == 0)
    def _():
        for k, piece in enumerate(pieces):
            for side in range(2):
                value = piece[side].astype(F32)
                value = jnp.concatenate(
                    [value, jnp.zeros((128 - rows, plan.cols), F32)], axis=0
                ).T
                start = (pair ^ k) * plan.pair_cols + (core if side == 0 else 1 - core) * plan.cols
                active[pl.ds(pl.multiple_of(start, 16), plan.cols), :] = value.astype(BF16)

    value = dot(matrix[0], active[...]).T + addend[pl.ds(step, 1), :]
    half = rows // 2
    first, second = value[:half], value[half:rows]
    mine[0] = jnp.where(core == 0, first, second)
    other[0] = jnp.where(core == 0, second, first)


def embed_kernel(plan, codes, table, resample, raising, placement, out, full):
    pair = lax.axis_index("tp") // 2
    row = lax.broadcasted_iota(jnp.int32, (plan.vocab, plan.lanes), 0)
    picked = (row == codes[...]).astype(F32)
    looked = dot(table[...], picked, precision=lax.Precision.HIGHEST)
    mapped = dot(looked, resample[...], precision=lax.Precision.HIGHEST).astype(BF16)
    fixed = placement[...].astype(F32)
    fixed = jnp.concatenate(
        [fixed, jnp.zeros((SLOT - plan.tokens, plan.width), F32)], axis=0
    )
    fixed = jnp.concatenate([fixed] * plan.pairs, axis=0).T
    full[...] = dot(raising[...], mapped, ((0,), (0,))) + fixed
    start = pl.multiple_of(pair * plan.pair_cols, 16)
    out[...] = full[pl.ds(start, plan.pair_cols), :].astype(BF16)


def layer_kernel(plan, tick, *refs):
    pairs = plan.pairs
    pieces = refs[:pairs]
    shifts = refs[pairs : 2 * pairs]
    mine, other, near, far, sharp, cached, attended, held = refs[2 * pairs : 2 * pairs + 8]
    normed, wide, scale_at, offset_at, qkv = refs[2 * pairs + 8 :]
    place = lax.axis_index("tp")
    core, pair = place % 2, place // 2
    step = pl.program_id(0)
    cols, pair_cols, dim = plan.cols, plan.pair_cols, plan.head_dim

    @pl.when(step == 0)
    def _():
        for k in range(pairs):
            at = pair ^ k
            if tick:
                start = pl.multiple_of(at * pair_cols, 16)
                wide[pl.ds(start, pair_cols), :] = pieces[k][...].astype(F32)
            for side in range(2):
                start = pl.multiple_of(
                    at * pair_cols + (core if side == 0 else 1 - core) * cols, 16
                )
                scale_at[pl.ds(start, cols), :] = spread(shifts[k][side, 0], tick, plan)
                offset_at[pl.ds(start, cols), :] = spread(shifts[k][side, 1], tick, plan)
        if tick == 0:
            blocks = [
                jnp.concatenate(
                    [
                        pieces[k][...].astype(F32),
                        jnp.zeros((SLOT - plan.tokens, plan.width), F32),
                    ],
                    axis=0,
                )
                for k in range(pairs)
            ]
            ordered = []
            for image in range(pairs):
                value = blocks[0]
                for k in range(1, pairs):
                    value = jnp.where((pair ^ k) == image, blocks[k], value)
                ordered.append(value)
            wide[...] = jnp.concatenate(ordered, axis=0).T
        value = wide[...]
        average = jnp.sum(value, axis=0, keepdims=True) * (1.0 / plan.width)
        centred = value - average
        spread_of = jnp.sum(centred * centred, axis=0, keepdims=True) * (1.0 / plan.width)
        result = centred * lax.rsqrt(spread_of + 1e-06) * (1.0 + scale_at[...]) + offset_at[...]
        normed[...] = result.astype(BF16)
        start = pl.multiple_of(pair * pair_cols, 16)
        held[...] = wide[pl.ds(start, pair_cols), :].astype(BF16)
        if plan.rows > pair_cols + plan.halo:
            qkv[:, pair_cols + plan.halo :, :] = jnp.zeros(
                (3, plan.rows - pair_cols - plan.halo, plan.lanes), BF16
            )

    tokens = normed[...]
    start = pl.multiple_of(core * cols, 16)
    qkv[step, pl.ds(start, cols), :] = dot(mine[0], tokens).astype(BF16)
    start = pl.multiple_of((1 - core) * cols, 16)
    qkv[step, pl.ds(start, cols), :] = dot(other[0], tokens).astype(BF16)
    edge = jnp.where(core == 1, near[0].astype(F32), far[0].astype(F32)).astype(BF16)
    qkv[step, pair_cols : pair_cols + plan.halo, :] = dot(edge, tokens).astype(BF16)

    @pl.when(step == 2)
    def _():
        head_at = first_head(pair, pair_cols, dim)
        begin = head_at * dim - pair * pair_cols
        lanes = plan.lanes
        row = lax.broadcasted_iota(jnp.int32, (lanes, lanes), 0)
        lane = lax.broadcasted_iota(jnp.int32, (lanes, lanes), 1)
        same = row // SLOT == lane // SLOT
        old_ok = same & (row % SLOT < plan.ctx)
        new_ok = same & (row % SLOT < plan.tokens)
        queries, keys, values, lifts, key_scales = [], [], [], [], []
        for head in range(plan.most):
            at = pl.ds(pl.multiple_of(begin + head * dim, 16), dim)
            query, key, value = qkv[0, at, :], qkv[1, at, :], qkv[2, at, :]
            wide_query, wide_key = query.astype(F32), key.astype(F32)
            lift = sharp[jnp.minimum(head_at + head, plan.heads - 1)]
            lifts.append(
                lax.rsqrt(jnp.sum(wide_query * wide_query, axis=0, keepdims=True) + 1e-06) * lift
            )
            key_scales.append(
                lax.rsqrt(jnp.sum(wide_key * wide_key, axis=0, keepdims=True) + 1e-06)
            )
            queries.append(query)
            keys.append(key)
            values.append(value)
        pad = -plan.most % 8
        stacked = key_scales + ([jnp.zeros((pad, lanes), F32)] if pad else [])
        key_cols = jnp.concatenate(stacked, axis=0).T
        old_keys = cached[:, 0, 0].reshape(lanes, plan.most * dim)
        old_values = cached[:, 1, 0].reshape(lanes, plan.most * dim)
        for head in range(plan.most):
            span = slice(head * dim, (head + 1) * dim)
            old = dot(old_keys[:, span], queries[head]) * lifts[head]
            new = (
                dot(keys[head], queries[head], ((0,), (0,)))
                * key_cols[:, head : head + 1]
                * lifts[head]
            )
            old = jnp.where(old_ok, old, -1e30)
            new = jnp.where(new_ok, new, -1e30)
            top = jnp.maximum(
                jnp.max(old, axis=0, keepdims=True), jnp.max(new, axis=0, keepdims=True)
            )
            old, new = jnp.exp(old - top), jnp.exp(new - top)
            total = jnp.sum(old, axis=0, keepdims=True) + jnp.sum(new, axis=0, keepdims=True)
            old, new = (old / total).astype(BF16), (new / total).astype(BF16)
            mixed = dot(old_values[:, span], old, ((0,), (0,))) + dot(values[head], new)
            attended[head * dim : (head + 1) * dim, :] = mixed.astype(BF16)


def return_kernel(plan, tick, *refs):
    pairs = plan.pairs
    pieces = refs[:pairs]
    mine, other, held, gate_mine, gate_other = refs[pairs : pairs + 5]
    rest = refs[pairs + 5 :]
    if tick == 0:
        entering, onward, rows, joined, projected, gate = rest
    else:
        rows, joined, projected, gate = rest
    place = lax.axis_index("tp")
    core, pair = place % 2, place // 2
    cols, pair_cols, dim = plan.cols, plan.pair_cols, plan.head_dim
    least = min(plan.counts)
    for k in range(pairs):
        at = pair ^ k
        start = first_head(at, pair_cols, dim)
        count = first_head(at + 1, pair_cols, dim) - start
        joined[pl.ds(pl.multiple_of(start * dim, 16), least * dim), :] = pieces[k][: least * dim, :]
        for extra in range(least, plan.most):

            @pl.when(count > extra)
            def _(k=k, extra=extra, start=start):
                joined[pl.ds(pl.multiple_of((start + extra) * dim, 16), dim), :] = pieces[k][
                    extra * dim : (extra + 1) * dim, :
                ]

    value = joined[...]
    for side, (matrix, gates) in enumerate(((mine, gate_mine), (other, gate_other))):
        start = pl.multiple_of((core if side == 0 else 1 - core) * cols, 16)
        projected[pl.ds(start, cols), :] = dot(matrix[...], value).astype(BF16).astype(F32)
        gate[pl.ds(start, cols), :] = spread(gates[...], tick, plan)
    result = held[...].astype(F32) + gate[...] * projected[...]
    turned = result.T
    for image in range(pairs):
        rows[image] = turned[image * SLOT : image * SLOT + plan.tokens, :].astype(BF16)
    if tick == 0:
        last = lax.axis_index("section") == plan.section - 1
        onward[...] = jnp.where(last, entering[...].astype(F32), result).astype(BF16)


def gather_kernel(plan, first, second, out):
    for tick, pieces in enumerate((first, second)):
        out[tick] = jnp.concatenate(
            [pieces[p].astype(F32) for p in range(plan.pairs)], axis=1
        ).astype(BF16)


def resample_blocks(plan):
    blocks = []
    for coarse in range(1, SIDE):
        fine = np.arange(SIDE, dtype=np.float32)
        rough = np.arange(coarse, dtype=np.float32)
        one = np.float32(1.0)
        size, parts = np.float32(SIDE), np.float32(coarse)
        begins = np.maximum(fine[:, None] / size, rough[None, :] / parts)
        finish = np.minimum((fine[:, None] + one) / size, (rough[None, :] + one) / parts)
        crossing = np.maximum(finish - begins, np.float32(0.0)) * size
        blocks.append(
            (crossing[:, None, :, None] * crossing[None, :, None, :]).reshape(
                SIDE * SIDE, coarse * coarse
            )
        )
    table = np.concatenate(blocks, axis=1).astype(np.float32)
    full = np.zeros((plan.lanes, plan.lanes), np.float32)
    for image in range(plan.pairs):
        at = image * SLOT
        full[at : at + table.shape[1], at : at + table.shape[0]] = table.T
    return full


def paired(plan, *args):
    (
        awaiting_arrivals,
        label_numbers,
        drawn_coarse_codes,
        discrete_prototypes,
        code_raising_operator,
        placement_tier_features,
        label_feature_rows,
        conditioned_gain_mapping,
        conditioned_shift_addend,
        question_answer_operator,
        mixing_return_operator,
        focus_sharpness_exponents,
        prior_resolution_probes,
        prior_resolution_answers,
    ) = args
    pairs, tp, cols, pair_cols = plan.pairs, plan.tp, plan.cols, plan.pair_cols
    width, lanes, dim, ticks = plan.width, plan.lanes, plan.head_dim, plan.ticks
    core = lax.axis_index("tp") % 2
    rows = ticks * plan.images
    half = rows // 2

    def across(value):
        return lax.ppermute(value, "tp", [(g, g ^ 1) for g in range(tp)])

    def around(value):
        return [value] + [
            lax.ppermute(value, "tp", [(g, g ^ (2 * k)) for g in range(tp)])
            for k in range(1, pairs)
        ]

    groups = [[2 * p + c for p in range(pairs)] for c in range(2)]

    def exchange(value):
        return lax.all_to_all(
            value, "tp", split_axis=0, concat_axis=0, tiled=True, axis_index_groups=groups
        )

    def call(kernel, out_shape, scratch, name, in_specs=None, **more):
        return pl.pallas_call(
            kernel,
            out_shape=out_shape,
            scratch_shapes=scratch,
            name=name,
            in_specs=in_specs,
            **more,
        )

    def struct(shape, dtype):
        return jax.ShapeDtypeStruct(shape, dtype)

    vmem, smem = whole(), whole(space=pltpu.SMEM)

    active = call(
        lambda *refs: label_kernel(plan, *refs),
        struct((rows, cols), BF16),
        [pltpu.VMEM((rows, plan.classes), F32)],
        "labels",
        [smem, vmem],
    )(label_numbers, label_feature_rows.T)
    active = around(jnp.stack([active, across(active)]))

    mod_matrix = jnp.transpose(conditioned_gain_mapping[0], (1, 2, 0))
    step_block = pl.BlockSpec((1, cols, width), lambda j: (j, 0, 0))
    out_block = pl.BlockSpec((1, half, cols), lambda j: (j, 0, 0))

    def fixed(shape):
        return pl.BlockSpec(shape, lambda j: (0,) * len(shape))

    mod_mine, mod_other = call(
        lambda *refs: modulation_kernel(plan, *refs),
        [struct((3, half, cols), F32)] * 2,
        [pltpu.VMEM((width, 128), BF16)],
        "modulation",
        [fixed((2, rows, cols))] * pairs + [step_block, fixed((3, cols))],
        grid=(3,),
        out_specs=[out_block, out_block],
    )(*active, mod_matrix, conditioned_shift_addend[0])
    mod_back = across(mod_other)
    shifts = around(jnp.stack([mod_mine[1:], mod_back[1:]]))

    qkv_mine = jnp.transpose(question_answer_operator[0], (1, 2, 0))
    qkv_other = across(qkv_mine)
    near = lax.ppermute(
        qkv_mine[:, : plan.halo],
        "tp",
        [(2 * p + 2, 2 * p + 1) for p in range(pairs) if plan.need[p]],
    )
    far = across(near)
    out_mine = mixing_return_operator[0].T
    out_other = across(out_mine)

    stored = jnp.stack([prior_resolution_probes[0, :, 0], prior_resolution_answers[0, :, 0]])
    span = plan.most * dim
    reach = max(plan.starts[p] * dim + span for p in range(pairs))
    stored = jnp.pad(
        stored, ((0, 0), (0, 0), (0, SLOT - plan.ctx), (0, max(0, reach - width)))
    )
    cached = exchange(
        jnp.stack([stored[..., plan.starts[p] * dim : plan.starts[p] * dim + span] for p in range(pairs)])
    )

    codes = lax.dynamic_index_in_dim(
        drawn_coarse_codes[0].reshape(pairs, 2, -1), core, 1, keepdims=False
    )
    codes = jnp.pad(codes, ((0, 0), (0, SLOT - plan.ctx))).reshape(1, lanes)
    entering = call(
        lambda *refs: embed_kernel(plan, *refs),
        struct((pair_cols, lanes), BF16),
        [pltpu.VMEM((width, lanes), F32)],
        "embed",
        [vmem] * 5,
    )(
        codes,
        discrete_prototypes.T,
        jnp.asarray(resample_blocks(plan)),
        code_raising_operator,
        placement_tier_features,
    )
    lifted = jnp.exp(jnp.minimum(focus_sharpness_exponents[0], LOG_CAP))

    emitted = []
    pieces = around(awaiting_arrivals[0, 0])
    for tick in range(ticks):
        cached_block = pl.BlockSpec(
            (pairs, 2, 1, SLOT, span), lambda j, tick=tick: (0, 0, tick, 0, 0)
        )
        halo_block = pl.BlockSpec((1, plan.halo, width), lambda j: (j, 0, 0))
        attended, held = call(
            lambda *refs, tick=tick: layer_kernel(plan, tick, *refs),
            [struct((span, lanes), BF16), struct((pair_cols, lanes), BF16)],
            [
                pltpu.VMEM((width, lanes), BF16),
                pltpu.VMEM((width, lanes), F32),
                pltpu.VMEM((width, lanes), F32),
                pltpu.VMEM((width, lanes), F32),
                pltpu.VMEM((3, plan.rows, lanes), BF16),
            ],
            f"layer_{tick}",
            [fixed(pieces[0].shape)] * pairs
            + [fixed(shifts[0].shape)] * pairs
            + [step_block, step_block, halo_block, halo_block, smem, cached_block],
            grid=(3,),
            out_specs=[fixed((span, lanes)), fixed((pair_cols, lanes))],
        )(*pieces, *shifts, qkv_mine, qkv_other, near, far, lifted, cached)
        outs = [struct((pairs, plan.tokens, pair_cols), BF16)]
        extra = []
        if tick + 1 < ticks:
            outs = [struct((pair_cols, lanes), BF16)] + outs
            extra = [entering]
        results = call(
            lambda *refs, tick=tick: return_kernel(plan, tick, *refs),
            outs,
            [
                pltpu.VMEM((width, lanes), BF16),
                pltpu.VMEM((pair_cols, lanes), F32),
                pltpu.VMEM((pair_cols, lanes), F32),
            ],
            f"return_{tick}",
            [vmem] * (pairs + 5 + len(extra)),
        )(*around(attended), out_mine, out_other, held, mod_mine[0], mod_back[0], *extra)
        if tick + 1 < ticks:
            onward = lax.ppermute(
                results[0], "section", [(s, (s + 1) % plan.section) for s in range(plan.section)]
            )
            pieces = around(onward)
        emitted.append(exchange(results[-1]))
    out = call(
        lambda *refs: gather_kernel(plan, *refs),
        struct((ticks, plan.tokens, width), BF16),
        [],
        "gather",
        [vmem, vmem],
    )(*emitted)
    return out[None, :, None]


def local(*args):
    plan = Plan(lax.axis_size("section"), lax.axis_size("tp"), args)
    return paired(plan, *args) if plan.fits else general(*args)


def solution(mesh):
    in_specs = (
        P("section", "tp", None, None),
        P(),
        P(),
        P(),
        P(),
        P(),
        P(None, "tp"),
        P("section", None, None, "tp"),
        P("section", None, "tp"),
        P("section", None, None, "tp"),
        P("section", None, "tp"),
        P("section", None),
        P("section", None, "tp", None, None),
        P("section", None, "tp", None, None),
    )
    out_specs = P("section", None, "tp", None, None)
    return jax.shard_map(local, mesh=mesh, in_specs=in_specs, out_specs=out_specs, check_vma=False)
```

```python
import jax
import jax.numpy as jnp
from jax import lax
from jax.experimental import pallas as pl
from jax.experimental.pallas import tpu as pltpu
from jax.sharding import PartitionSpec as P
import numpy as np

FOCUS_GROUPS = 30
HEAD_DIM = 64
SIDE = 5


LOG_CAP = 4.605170185988092


def shifted(value, axis, steps):
    count = lax.axis_size(axis)
    first, last = (max(0, -steps), min(count, count - steps))
    return lax.ppermute(value, axis, [(source, source + steps) for source in range(first, last)])


def crossing_matrix(target, coarse):
    fine_index = jnp.arange(target, dtype=jnp.float32)
    coarse_index = jnp.arange(coarse, dtype=jnp.float32)
    begins = jnp.maximum(fine_index[:, None] / target, coarse_index[None, :] / coarse)
    finish = jnp.minimum(
        (fine_index[:, None] + 1.0) / target, (coarse_index[None, :] + 1.0) / coarse
    )
    return jnp.maximum(finish - begins, 0.0) * target


def resampler():
    blocks = []
    for coarse in range(1, SIDE):
        crossing = crossing_matrix(SIDE, coarse)
        blocks.append(
            (crossing[:, None, :, None] * crossing[None, :, None, :]).reshape(
                SIDE * SIDE, coarse * coarse
            )
        )
    return jnp.concatenate(blocks, axis=1)


def embed(
    drawn_coarse_codes,
    discrete_prototypes,
    code_raising_operator,
    placement_tier_features,
    resample_table,
):
    looked_up = discrete_prototypes[drawn_coarse_codes]
    mapped = jnp.einsum(
        "tc,nicv->nitv", resample_table, looked_up, precision=lax.Precision.HIGHEST
    ).astype(jnp.bfloat16)
    leading = mapped.shape[:3]
    projected_rows = jnp.dot(
        mapped.reshape(-1, mapped.shape[3]),
        code_raising_operator,
        preferred_element_type=jnp.float32,
    )
    projected_rows = projected_rows.reshape(leading + (code_raising_operator.shape[1],))
    return (projected_rows + placement_tier_features.astype(jnp.float32)).astype(jnp.bfloat16)


def norm_mod(latent_stream, scale_term, offset_term):
    widened = latent_stream.astype(jnp.float32)
    average = jnp.mean(widened, axis=-1, keepdims=True)
    centred = widened - average
    spread = jnp.mean(centred * centred, axis=-1, keepdims=True)
    normed = (
        centred * lax.rsqrt(spread + 1e-06) * (1.0 + scale_term[:, None, :])
        + offset_term[:, None, :]
    )
    return normed.astype(jnp.bfloat16)


def attention(qkv_cols, log_scale, cached_keys, cached_values):
    qkv = lax.all_to_all(qkv_cols, "tp", split_axis=0, concat_axis=3, tiled=True)
    images = qkv.shape[0]
    count = qkv.shape[1]
    widened = qkv.astype(jnp.float32)
    query = widened[:, :, 0].reshape(images, count, FOCUS_GROUPS, HEAD_DIM)
    new_keys = widened[:, :, 1].reshape(images, count, FOCUS_GROUPS, HEAD_DIM)
    new_values = qkv[:, :, 2].reshape(images, count, FOCUS_GROUPS, HEAD_DIM)
    head_mult = jnp.exp(jnp.minimum(log_scale, LOG_CAP))
    query = (
        query
        * lax.rsqrt(jnp.sum(query * query, axis=-1, keepdims=True) + 1e-06)
        * head_mult[:, None]
    )
    new_keys = new_keys * lax.rsqrt(jnp.sum(new_keys * new_keys, axis=-1, keepdims=True) + 1e-06)
    all_keys = jnp.concatenate(
        [cached_keys.astype(jnp.float32).reshape(images, -1, FOCUS_GROUPS, HEAD_DIM), new_keys],
        axis=1,
    )
    all_values = jnp.concatenate(
        [cached_values.reshape(images, -1, FOCUS_GROUPS, HEAD_DIM), new_values], axis=1
    )
    scores = jnp.einsum("iqhd,ikhd->ihqk", query, all_keys, precision=lax.Precision.HIGHEST)
    maximum = jnp.max(scores, axis=-1, keepdims=True)
    weights = jnp.exp(scores - maximum)
    probabilities = (weights / jnp.sum(weights, axis=-1, keepdims=True)).astype(jnp.bfloat16)
    mixed = jnp.einsum(
        "ihqk,ikhd->iqhd", probabilities, all_values, preferred_element_type=jnp.float32
    )
    return mixed.reshape(images, count, FOCUS_GROUPS * HEAD_DIM).astype(jnp.bfloat16)


def project_out(attended, out_matrix):
    return jnp.dot(
        lax.all_gather(attended, "tp", axis=0, tiled=True),
        out_matrix,
        preferred_element_type=jnp.float32,
    )


def pass_on(latent_stream):
    return shifted(latent_stream, "section", 1)


def general(
    awaiting_arrivals,
    label_numbers,
    drawn_coarse_codes,
    discrete_prototypes,
    code_raising_operator,
    placement_tier_features,
    label_feature_rows,
    conditioned_gain_mapping,
    conditioned_shift_addend,
    question_answer_operator,
    mixing_return_operator,
    focus_sharpness_exponents,
    prior_resolution_probes,
    prior_resolution_answers,
):
    sections = lax.axis_size("section")
    section_at = lax.axis_index("section")
    group_index = lax.axis_index("tp")
    moments = prior_resolution_probes.shape[1]
    width = question_answer_operator.shape[1]
    column_width = question_answer_operator.shape[3]
    images = drawn_coarse_codes.shape[1]
    resident_pictures = awaiting_arrivals.shape[1]
    class_rows = lax.dynamic_slice_in_dim(label_numbers, sections - 1 - section_at, moments, 0)
    class_part = jnp.take(label_feature_rows, class_rows, axis=0)
    activated_part = jax.nn.silu(class_part.astype(jnp.float32)).astype(jnp.bfloat16)
    gated_response = lax.all_gather(activated_part, "tp", axis=2, tiled=True)
    flat_active = gated_response.reshape(moments * images, width)
    inner_block = 0
    local_mod = conditioned_gain_mapping[inner_block].reshape(width, 3 * column_width)
    modulated = jnp.dot(flat_active, local_mod, preferred_element_type=jnp.float32)
    mod_list = [
        modulated.reshape(moments, images, 3, column_width) + conditioned_shift_addend[inner_block]
    ]
    mod_cols = jnp.stack(mod_list)
    resample_table = resampler()
    emitted = []
    mod_rows = lax.all_to_all(mod_cols, "tp", split_axis=2, concat_axis=4, tiled=True)
    own_tokens = lax.dynamic_slice_in_dim(
        drawn_coarse_codes, group_index * resident_pictures, resident_pictures, 1
    )
    entering = embed(
        own_tokens,
        discrete_prototypes,
        code_raising_operator,
        placement_tier_features,
        resample_table,
    )
    passed_along_activation = awaiting_arrivals[0]
    for clock_tick in range(moments):
        latent_stream = passed_along_activation
        inner_block = 0
        modulation = mod_rows[inner_block, clock_tick]
        normed = norm_mod(latent_stream, modulation[:, 1], modulation[:, 2])
        local_qkv = question_answer_operator[inner_block].reshape(width, 3 * column_width)

        def body_product(portion, offset, local_qkv=local_qkv):
            return jnp.dot(portion, local_qkv, preferred_element_type=jnp.float32).astype(
                jnp.bfloat16
            )

        qkv_cols = body_product(lax.all_gather(normed, "tp", axis=0, tiled=True), jnp.int32(0))
        qkv_cols = qkv_cols.reshape(qkv_cols.shape[0], qkv_cols.shape[1], 3, column_width)
        attended = attention(
            qkv_cols,
            focus_sharpness_exponents[inner_block],
            prior_resolution_probes[inner_block, clock_tick],
            prior_resolution_answers[inner_block, clock_tick],
        )
        projected_cols = project_out(attended, mixing_return_operator[inner_block]).astype(
            jnp.bfloat16
        )
        projected = lax.all_to_all(projected_cols, "tp", split_axis=0, concat_axis=2, tiled=True)
        latent_stream = (
            latent_stream.astype(jnp.float32)
            + modulation[:, 0][:, None, :] * projected.astype(jnp.float32)
        ).astype(jnp.bfloat16)
        emitted.append(latent_stream)
        if clock_tick + 1 < moments:
            arrived = pass_on(latent_stream)
            passed_along_activation = jnp.where(section_at == 0, entering[clock_tick], arrived)
    result = jnp.stack(emitted)
    return result[None]


SLOT = 32
F32 = jnp.float32
BF16 = jnp.bfloat16
KERNEL_VMEM = 16 * 1024 * 1024


def first_head(pair, pair_width, head_dim):
    return (2 * pair * pair_width + head_dim) // (2 * head_dim)


class Plan:
    def __init__(self, section, tp, args):
        (arrivals, _, codes, prototypes, _, placement, labels, gain, _, _, _, sharp, probes, _) = args
        self.section, self.tp = section, tp
        self.pairs = tp // 2
        self.width = gain.shape[1]
        self.cols = gain.shape[3]
        self.pair_cols = 2 * self.cols
        self.heads = sharp.shape[1]
        self.head_dim = self.width // self.heads
        self.tokens = placement.shape[0]
        self.ctx = probes.shape[3]
        self.ticks = probes.shape[1]
        self.images = codes.shape[1]
        self.resident = arrivals.shape[1]
        self.lanes = self.pairs * SLOT
        self.classes = labels.shape[0]
        self.vocab, self.code_dim = prototypes.shape
        starts = [first_head(p, self.pair_cols, self.head_dim) for p in range(self.pairs + 1)]
        self.starts = starts
        self.counts = [starts[p + 1] - starts[p] for p in range(self.pairs)]
        self.most = max(self.counts)
        self.left = [p * self.pair_cols - starts[p] * self.head_dim for p in range(self.pairs)]
        self.need = [
            max(0, starts[p + 1] * self.head_dim - (p + 1) * self.pair_cols)
            for p in range(self.pairs)
        ]
        self.halo = max(self.need)
        self.rows = max(self.pair_cols + self.halo, self.most * self.head_dim - min(self.left))
        self.fits = (
            tp % 2 == 0
            and self.pairs & (self.pairs - 1) == 0
            and gain.shape[0] == 1
            and codes.shape[0] == 1
            and self.ticks == 2
            and self.resident == 1
            and self.images == tp
            and self.cols % 16 == 0
            and self.head_dim == HEAD_DIM
            and starts[-1] == self.heads
            and max(self.left) <= 0
            and all(offset % 16 == 0 for offset in self.left)
            and 0 < self.halo <= self.cols
            and self.halo % 16 == 0
            and self.tokens <= SLOT
            and self.ctx <= SLOT
            and self.lanes == 128
        )


def dot(left, right, contract=((1,), (0,)), precision=None):
    return lax.dot_general(
        left, right, (contract, ((), ())), preferred_element_type=F32, precision=precision
    )


def spread(rows, tick, plan):
    part = rows[tick * plan.pairs : (tick + 1) * plan.pairs, :]
    parts = []
    for _ in range(3):
        rounded = part.astype(BF16).astype(F32)
        parts.append(rounded)
        part = part - rounded
    count = 3 * plan.pairs
    stacked = jnp.concatenate(parts, axis=0).astype(BF16)
    row = lax.broadcasted_iota(jnp.int32, (count, plan.lanes), 0)
    lane = lax.broadcasted_iota(jnp.int32, (count, plan.lanes), 1)
    pick = (row % plan.pairs == lane // SLOT).astype(F32).astype(BF16)
    return dot(stacked, pick, ((0,), (0,)))


def label_kernel(plan, labels, table, out, picked):
    section_at = lax.axis_index("section")
    place = lax.broadcasted_iota(jnp.int32, (1, plan.classes), 1)
    row = 0
    for core in range(2):
        for tick in range(plan.ticks):
            for pair in range(plan.pairs):
                label = labels[tick - section_at + plan.section - 1, 2 * pair + core]
                picked[row : row + 1, :] = (place == label).astype(F32)
                row += 1
    value = dot(picked[...].astype(BF16), table[...], ((1,), (1,)))
    out[...] = (value / (1.0 + jnp.exp(-value))).astype(BF16)


def modulation_kernel(plan, *refs):
    pairs = plan.pairs
    near, far = refs[:pairs], refs[pairs : 2 * pairs]
    matrix, addend, shift, gate, active = refs[2 * pairs :]
    place = lax.axis_index("tp")
    core, pair = place % 2, place // 2
    rows = plan.ticks * plan.images
    for k in range(pairs):
        for side, piece in enumerate((near[k], far[k])):
            value = piece[...].astype(F32)
            value = jnp.concatenate([value, jnp.zeros((128 - rows, plan.cols), F32)], axis=0).T
            start = (pair ^ k) * plan.pair_cols + (core if side == 0 else 1 - core) * plan.cols
            active[pl.ds(pl.multiple_of(start, 16), plan.cols), :] = value.astype(BF16)
    tokens = active[...]
    for part in range(3):
        value = dot(matrix[part], tokens).T[:rows] + addend[part]
        if part:
            shift[part - 1] = value
        else:
            gate[...] = value


def packed_rows(plan):
    up = lambda rows: rows + -rows % 8
    first = up(plan.pairs * plan.tokens)
    second = first + up(plan.ctx)
    return first, second, second + up(plan.ctx)


def stored_kernel(plan, arrival, probes, answers, matrix, edge, *outs):
    pairs = plan.pairs
    pair = lax.axis_index("tp") // 2
    span = plan.most * plan.head_dim
    key_at, value_at, _ = packed_rows(plan)
    early, late = outs[:pairs], outs[pairs:]
    edge[...] = matrix[:, : plan.halo, :]
    wide = arrival[...].astype(F32)
    wide_keys, wide_values = probes[...].astype(F32), answers[...].astype(F32)
    keys = [wide_keys[:, tick, :] for tick in range(plan.ticks)]
    values = [wide_values[:, tick, :] for tick in range(plan.ticks)]
    chunks = []
    for at in range(pairs):
        chunk = wide[:, at * plan.pair_cols : (at + 1) * plan.pair_cols]
        chunks.append(
            jnp.concatenate([chunk, jnp.zeros((plan.tokens, span - plan.pair_cols), F32)], axis=1)
        )
    top = jnp.concatenate(
        chunks + [jnp.zeros((key_at - pairs * plan.tokens, span), F32)], axis=0
    ).astype(BF16)

    def cut(value, at, rows):
        start = plan.starts[at] * plan.head_dim
        reach = min(span, plan.width - start)
        part = value[:, start : start + reach]
        if reach < span:
            part = jnp.concatenate([part, jnp.zeros((plan.ctx, span - reach), F32)], axis=1)
        return jnp.concatenate([part, jnp.zeros((rows - plan.ctx, span), F32)], axis=0).astype(BF16)

    for k in range(pairs):
        early[k][:key_at, :] = top
    for at in range(pairs):
        pieces = [
            cut(keys[0], at, value_at - key_at),
            cut(values[0], at, value_at - key_at),
            cut(keys[1], at, SLOT),
            cut(values[1], at, SLOT),
        ]
        for k in range(pairs):

            @pl.when((pair ^ k) == at)
            def _(k=k, pieces=pieces):
                early[k][key_at:value_at, :] = pieces[0]
                early[k][value_at:, :] = pieces[1]
                late[k][0], late[k][1] = pieces[2], pieces[3]


def embed_kernel(plan, codes, table, resample, raising, placement, out, full):
    place = lax.axis_index("tp")
    core, pair = place % 2, place // 2
    row = lax.broadcasted_iota(jnp.int32, (plan.vocab, plan.lanes), 0)
    blank = jnp.zeros((1, SLOT - plan.ctx), jnp.int32)
    slots = []
    for image in range(plan.pairs):
        both = codes[2 * image : 2 * image + 2, :]
        slots += [jnp.where(core == 0, both[:1], both[1:]), blank]
    picked = (row == jnp.concatenate(slots, axis=1)).astype(F32)
    looked = dot(table[...], picked, precision=lax.Precision.HIGHEST)
    mapped = dot(looked, resample[...], precision=lax.Precision.HIGHEST).astype(BF16)
    fixed = placement[...].astype(F32)
    fixed = jnp.concatenate(
        [fixed, jnp.zeros((SLOT - plan.tokens, plan.width), F32)], axis=0
    )
    fixed = jnp.concatenate([fixed] * plan.pairs, axis=0).T
    full[...] = dot(raising[...], mapped, ((0,), (0,))) + fixed
    start = pl.multiple_of(pair * plan.pair_cols, 16)
    out[...] = full[pl.ds(start, plan.pair_cols), :].astype(BF16)


def layer_kernel(plan, tick, *refs):
    pairs = plan.pairs
    pieces = refs[:pairs]
    shifts = (refs[pairs : 2 * pairs], refs[2 * pairs : 3 * pairs])
    stores = refs[3 * pairs : 4 * pairs] if tick else None
    refs = refs[4 * pairs :] if tick else refs[3 * pairs :]
    mine, other, near, far, sharp, attended, held = refs[:7]
    wide, scale_at, offset_at, qkv, cached, *turning = refs[7:]
    half = plan.ticks * plan.pairs
    place = lax.axis_index("tp")
    core, pair = place % 2, place // 2
    cols, pair_cols, dim, lanes = plan.cols, plan.pair_cols, plan.head_dim, plan.lanes

    for k in range(pairs):
        at = pair ^ k
        slot = pl.multiple_of(at * SLOT, SLOT)
        if tick:
            start = pl.multiple_of(at * pair_cols, 16)
            wide[pl.ds(start, pair_cols), :] = pieces[k][...].astype(F32)
            cached[0, pl.ds(slot, SLOT), :] = stores[k][0]
            cached[1, pl.ds(slot, SLOT), :] = stores[k][1]
        else:
            key_at, value_at, _ = packed_rows(plan)
            packed = pieces[k][...].astype(F32)
            chunks = [
                packed[j * plan.tokens : (j + 1) * plan.tokens, :pair_cols] for j in range(pairs)
            ]
            turning[0][pl.ds(slot, SLOT), :] = jnp.concatenate(
                [
                    jnp.concatenate(chunks, axis=1),
                    jnp.zeros((SLOT - plan.tokens, plan.width), F32),
                ],
                axis=0,
            )
            cached[0, pl.ds(slot, value_at - key_at), :] = packed[key_at:value_at].astype(BF16)
            cached[1, pl.ds(slot, value_at - key_at), :] = packed[value_at:].astype(BF16)
        for side in range(2):
            start = pl.multiple_of(
                at * pair_cols + (core if side == 0 else 1 - core) * cols, 16
            )
            own = pl.ds(pl.multiple_of(core * half, 8), half)
            scale_at[pl.ds(start, cols), :] = spread(shifts[side][k][0, own, :], tick, plan)
            offset_at[pl.ds(start, cols), :] = spread(shifts[side][k][1, own, :], tick, plan)
    if tick == 0:
        wide[...] = turning[0][...].T
    value = wide[...]
    average = jnp.sum(value, axis=0, keepdims=True) * (1.0 / plan.width)
    centred = value - average
    variance = jnp.sum(centred * centred, axis=0, keepdims=True) * (1.0 / plan.width)
    result = centred * lax.rsqrt(variance + 1e-06) * (1.0 + scale_at[...]) + offset_at[...]
    tokens = result.astype(BF16)
    start = pl.multiple_of(pair * pair_cols, 16)
    held[...] = wide[pl.ds(start, pair_cols), :].astype(BF16)
    if plan.rows > pair_cols + plan.halo:
        qkv[:, pair_cols + plan.halo :, :] = jnp.zeros(
            (3, plan.rows - pair_cols - plan.halo, lanes), BF16
        )
    for part in range(3):
        start = pl.multiple_of(core * cols, 16)
        qkv[part, pl.ds(start, cols), :] = dot(mine[part], tokens).astype(BF16)
        start = pl.multiple_of((1 - core) * cols, 16)
        qkv[part, pl.ds(start, cols), :] = dot(other[part], tokens).astype(BF16)
        edge = jnp.where(core == 1, near[part].astype(F32), far[part].astype(F32)).astype(BF16)
        qkv[part, pair_cols : pair_cols + plan.halo, :] = dot(edge, tokens).astype(BF16)

    head_at = first_head(pair, pair_cols, dim)
    begin = head_at * dim - pair * pair_cols
    row = lax.broadcasted_iota(jnp.int32, (lanes, lanes), 0)
    lane = lax.broadcasted_iota(jnp.int32, (lanes, lanes), 1)
    same = row // SLOT == lane // SLOT
    old_ok = same & (row % SLOT < plan.ctx)
    new_ok = same & (row % SLOT < plan.tokens)
    queries, keys, values, lifts, key_scales = [], [], [], [], []
    for head in range(plan.most):
        at = pl.ds(pl.multiple_of(begin + head * dim, 16), dim)
        query, key, value = qkv[0, at, :], qkv[1, at, :], qkv[2, at, :]
        wide_query, wide_key = query.astype(F32), key.astype(F32)
        lift = sharp[0, jnp.minimum(head_at + head, plan.heads - 1)]
        lift = jnp.exp(jnp.minimum(jnp.full((1, lanes), lift, F32), LOG_CAP))
        lifts.append(
            lax.rsqrt(jnp.sum(wide_query * wide_query, axis=0, keepdims=True) + 1e-06) * lift
        )
        key_scales.append(lax.rsqrt(jnp.sum(wide_key * wide_key, axis=0, keepdims=True) + 1e-06))
        queries.append(query)
        keys.append(key)
        values.append(value)
    pad = -plan.most % 8
    key_cols = jnp.concatenate(
        key_scales + ([jnp.zeros((pad, lanes), F32)] if pad else []), axis=0
    ).T
    old_keys, old_values = cached[0], cached[1]
    for head in range(plan.most):
        span = slice(head * dim, (head + 1) * dim)
        old = dot(old_keys[:, span], queries[head]) * lifts[head]
        new = (
            dot(keys[head], queries[head], ((0,), (0,)))
            * key_cols[:, head : head + 1]
            * lifts[head]
        )
        old = jnp.where(old_ok, old, -1e30)
        new = jnp.where(new_ok, new, -1e30)
        top = jnp.maximum(
            jnp.max(old, axis=0, keepdims=True), jnp.max(new, axis=0, keepdims=True)
        )
        old, new = jnp.exp(old - top), jnp.exp(new - top)
        total = 1.0 / (jnp.sum(old, axis=0, keepdims=True) + jnp.sum(new, axis=0, keepdims=True))
        old, new = (old * total).astype(BF16), (new * total).astype(BF16)
        mixed = dot(old_values[:, span], old, ((0,), (0,))) + dot(values[head], new)
        attended[head * dim : (head + 1) * dim, :] = mixed.astype(BF16)


def return_kernel(plan, tick, *refs):
    pairs = plan.pairs
    pieces = refs[:pairs]
    mine, other, held, gate_mine, gate_other = refs[pairs : pairs + 5]
    rest = refs[pairs + 5 :]
    if tick == 0:
        entering, onward, *rows = rest[:-3]
    else:
        rows = rest[:-3]
    joined, projected, gate = rest[-3:]
    place = lax.axis_index("tp")
    core, pair = place % 2, place // 2
    cols, pair_cols, dim = plan.cols, plan.pair_cols, plan.head_dim
    least = min(plan.counts)
    half = plan.ticks * pairs
    for k in range(pairs):
        at = pair ^ k
        start = first_head(at, pair_cols, dim)
        count = first_head(at + 1, pair_cols, dim) - start
        joined[pl.ds(pl.multiple_of(start * dim, 16), least * dim), :] = pieces[k][: least * dim, :]
        for extra in range(least, plan.most):

            @pl.when(count > extra)
            def _(k=k, extra=extra, start=start):
                joined[pl.ds(pl.multiple_of((start + extra) * dim, 16), dim), :] = pieces[k][
                    extra * dim : (extra + 1) * dim, :
                ]

    value = joined[...]
    for side, (matrix, gates) in enumerate(((mine, gate_mine), (other, gate_other))):
        start = pl.multiple_of((core if side == 0 else 1 - core) * cols, 16)
        projected[pl.ds(start, cols), :] = dot(matrix[...], value).astype(BF16).astype(F32)
        gates = gates[pl.ds(pl.multiple_of(core * half, 8), half), :]
        gate[pl.ds(start, cols), :] = spread(gates, tick, plan)
    result = held[...].astype(F32) + gate[...] * projected[...]
    turned = result.T
    for k in range(pairs):
        for image in range(pairs):

            @pl.when((pair ^ k) == image)
            def _(k=k, image=image):
                rows[k][...] = turned[image * SLOT : image * SLOT + plan.tokens, :].astype(BF16)

    if tick == 0:
        last = lax.axis_index("section") == plan.section - 1
        onward[...] = jnp.where(last, entering[...].astype(F32), result).astype(BF16)


def gather_kernel(plan, *refs):
    pairs = plan.pairs
    pieces, out, full = refs[:-2], refs[-2], refs[-1]
    pair = lax.axis_index("tp") // 2
    for tick in range(plan.ticks):
        for k in range(pairs):
            for at in range(pairs):

                @pl.when((pair ^ k) == at)
                def _(tick=tick, k=k, at=at):
                    full[tick, :, at * plan.pair_cols : (at + 1) * plan.pair_cols] = pieces[
                        tick * pairs + k
                    ][...].astype(F32)

    for tick in range(plan.ticks):
        out[tick] = full[tick].astype(BF16)


def resample_blocks(plan):
    blocks = []
    for coarse in range(1, SIDE):
        fine = np.arange(SIDE, dtype=np.float32)
        rough = np.arange(coarse, dtype=np.float32)
        one = np.float32(1.0)
        size, parts = np.float32(SIDE), np.float32(coarse)
        begins = np.maximum(fine[:, None] / size, rough[None, :] / parts)
        finish = np.minimum((fine[:, None] + one) / size, (rough[None, :] + one) / parts)
        crossing = np.maximum(finish - begins, np.float32(0.0)) * size
        blocks.append(
            (crossing[:, None, :, None] * crossing[None, :, None, :]).reshape(
                SIDE * SIDE, coarse * coarse
            )
        )
    table = np.concatenate(blocks, axis=1).astype(np.float32)
    full = np.zeros((plan.lanes, plan.lanes), np.float32)
    for image in range(plan.pairs):
        at = image * SLOT
        full[at : at + table.shape[1], at : at + table.shape[0]] = table.T
    return full


def paired(plan, *args):
    (
        awaiting_arrivals,
        label_numbers,
        drawn_coarse_codes,
        discrete_prototypes,
        code_raising_operator,
        placement_tier_features,
        label_feature_rows,
        conditioned_gain_mapping,
        conditioned_shift_addend,
        question_answer_operator,
        mixing_return_operator,
        focus_sharpness_exponents,
        prior_resolution_probes,
        prior_resolution_answers,
    ) = args
    pairs, tp, cols, pair_cols = plan.pairs, plan.tp, plan.cols, plan.pair_cols
    width, lanes, dim, ticks = plan.width, plan.lanes, plan.head_dim, plan.ticks
    rows = ticks * plan.images

    def swap(value, k):
        return lax.ppermute(value, "tp", [(g, g ^ (2 * k)) for g in range(tp)])

    def across(value):
        return lax.ppermute(value, "tp", [(g, g ^ 1) for g in range(tp)])

    def around(value):
        return [value] + [swap(value, k) for k in range(1, pairs)]

    def call(kernel, outs, scratch, values, scalars=(), loose=()):
        ins = [
            pltpu.with_memory_space_constraint(
                v, pltpu.HBM if i in scalars or i in loose else pltpu.VMEM
            )
            for i, v in enumerate(values)
        ]
        return pl.pallas_call(
            lambda *refs: kernel(plan, *refs),
            out_shape=[pltpu.VMEM(shape, dtype) for shape, dtype in outs],
            in_specs=[
                pl.BlockSpec(memory_space=pltpu.SMEM if i in scalars else pltpu.VMEM)
                for i in range(len(values))
            ],
            out_specs=[pl.BlockSpec(memory_space=pltpu.VMEM)] * len(outs),
            scratch_shapes=scratch,
            compiler_params=pltpu.CompilerParams(vmem_limit_bytes=KERNEL_VMEM),
        )(*ins)

    span = plan.most * dim
    (active,) = call(
        label_kernel,
        [((rows, cols), BF16)],
        [pltpu.VMEM((rows, plan.classes), F32)],
        [label_numbers, label_feature_rows.T],
        (0,),
        (1,),
    )
    active = around(active)
    active += [across(piece) for piece in active]
    shift, gate = call(
        modulation_kernel,
        [((2, rows, cols), F32), ((rows, cols), F32)],
        [pltpu.VMEM((width, 128), BF16)],
        [
            *active,
            jnp.transpose(conditioned_gain_mapping[0], (1, 2, 0)),
            jnp.transpose(conditioned_shift_addend, (1, 0, 2)),
        ],
    )
    shifts = around(shift)
    shifts += [across(piece) for piece in shifts]
    gate_back = across(gate)

    qkv_mine = jnp.transpose(question_answer_operator[0], (1, 2, 0))
    qkv_other = across(qkv_mine)
    out_mine = mixing_return_operator[0].T
    out_other = across(out_mine)
    edge, *stores = call(
        stored_kernel,
        [((3, plan.halo, width), BF16)]
        + [((packed_rows(plan)[2], span), BF16)] * pairs
        + [((2, SLOT, span), BF16)] * pairs,
        [],
        [
            awaiting_arrivals[0, 0],
            jnp.transpose(prior_resolution_probes[0, :, 0], (1, 0, 2)),
            jnp.transpose(prior_resolution_answers[0, :, 0], (1, 0, 2)),
            qkv_mine,
        ],
        (),
        (0, 1, 2),
    )
    near = lax.ppermute(edge, "tp", [(2 * p + 2, 2 * p + 1) for p in range(pairs) if plan.need[p]])
    far = across(near)
    pieces = [stores[0]] + [swap(stores[k], k) for k in range(1, pairs)]
    later = [stores[pairs]] + [swap(stores[pairs + k], k) for k in range(1, pairs)]
    (entering,) = call(
        embed_kernel,
        [((pair_cols, lanes), BF16)],
        [pltpu.VMEM((width, lanes), F32)],
        [
            drawn_coarse_codes[0],
            discrete_prototypes.T,
            jnp.asarray(resample_blocks(plan)),
            code_raising_operator,
            placement_tier_features,
        ],
        (),
        range(5),
    )

    emitted = []
    for tick in range(ticks):
        scratch = [
            pltpu.VMEM((width, lanes), F32),
            pltpu.VMEM((width, lanes), F32),
            pltpu.VMEM((width, lanes), F32),
            pltpu.VMEM((3, plan.rows, lanes), BF16),
            pltpu.VMEM((2, lanes, span), BF16),
        ]
        if tick == 0:
            scratch.append(pltpu.VMEM((lanes, width), F32))
        values = [*pieces, *shifts] + (later if tick else [])
        values += [qkv_mine, qkv_other, near, far, focus_sharpness_exponents]
        attended, held = call(
            lambda *refs, tick=tick: layer_kernel(refs[0], tick, *refs[1:]),
            [((span, lanes), BF16), ((pair_cols, lanes), BF16)],
            scratch,
            values,
            (len(values) - 1,),
        )
        outs = [((plan.tokens, pair_cols), BF16)] * pairs
        extra = []
        if tick + 1 < ticks:
            outs = [((pair_cols, lanes), BF16)] + outs
            extra = [entering]
        results = call(
            lambda *refs, tick=tick: return_kernel(refs[0], tick, *refs[1:]),
            outs,
            [
                pltpu.VMEM((width, lanes), BF16),
                pltpu.VMEM((pair_cols, lanes), F32),
                pltpu.VMEM((pair_cols, lanes), F32),
            ],
            [
                *around(attended),
                out_mine,
                out_other,
                held,
                gate,
                gate_back,
                *extra,
            ],
        )
        if tick + 1 < ticks:
            onward = lax.ppermute(
                results[0],
                "section",
                [(s, (s + 1) % plan.section) for s in range(plan.section)],
            )
            pieces = around(onward)
        final = results[-pairs:]
        emitted += [final[0]] + [swap(final[k], k) for k in range(1, pairs)]
    (out,) = call(
        gather_kernel,
        [((ticks, plan.tokens, width), BF16)],
        [pltpu.VMEM((ticks, plan.tokens, width), F32)],
        emitted,
    )
    return out[None, :, None]


def local(*args):
    plan = Plan(lax.axis_size("section"), lax.axis_size("tp"), args)
    return paired(plan, *args) if plan.fits else general(*args)


def solution(mesh):
    in_specs = (
        P("section", "tp", None, None),
        P(),
        P(),
        P(),
        P(),
        P(),
        P(None, "tp"),
        P("section", None, None, "tp"),
        P("section", None, "tp"),
        P("section", None, None, "tp"),
        P("section", None, "tp"),
        P("section", None),
        P("section", None, "tp", None, None),
        P("section", None, "tp", None, None),
    )
    out_specs = P("section", None, "tp", None, None)
    return jax.shard_map(local, mesh=mesh, in_specs=in_specs, out_specs=out_specs, check_vma=False)
```

```python
import jax
import jax.numpy as jnp
from jax import lax
from jax.experimental import pallas as pl
from jax.experimental.pallas import tpu as pltpu
from jax.sharding import PartitionSpec as P
import numpy as np

FOCUS_GROUPS = 30
HEAD_DIM = 64
SIDE = 5


LOG_CAP = 4.605170185988092


def shifted(value, axis, steps):
    count = lax.axis_size(axis)
    first, last = (max(0, -steps), min(count, count - steps))
    return lax.ppermute(value, axis, [(source, source + steps) for source in range(first, last)])


def crossing_matrix(target, coarse):
    fine_index = jnp.arange(target, dtype=jnp.float32)
    coarse_index = jnp.arange(coarse, dtype=jnp.float32)
    begins = jnp.maximum(fine_index[:, None] / target, coarse_index[None, :] / coarse)
    finish = jnp.minimum(
        (fine_index[:, None] + 1.0) / target, (coarse_index[None, :] + 1.0) / coarse
    )
    return jnp.maximum(finish - begins, 0.0) * target


def resampler():
    blocks = []
    for coarse in range(1, SIDE):
        crossing = crossing_matrix(SIDE, coarse)
        blocks.append(
            (crossing[:, None, :, None] * crossing[None, :, None, :]).reshape(
                SIDE * SIDE, coarse * coarse
            )
        )
    return jnp.concatenate(blocks, axis=1)


def embed(
    drawn_coarse_codes,
    discrete_prototypes,
    code_raising_operator,
    placement_tier_features,
    resample_table,
):
    looked_up = discrete_prototypes[drawn_coarse_codes]
    mapped = jnp.einsum(
        "tc,nicv->nitv", resample_table, looked_up, precision=lax.Precision.HIGHEST
    ).astype(jnp.bfloat16)
    leading = mapped.shape[:3]
    projected_rows = jnp.dot(
        mapped.reshape(-1, mapped.shape[3]),
        code_raising_operator,
        preferred_element_type=jnp.float32,
    )
    projected_rows = projected_rows.reshape(leading + (code_raising_operator.shape[1],))
    return (projected_rows + placement_tier_features.astype(jnp.float32)).astype(jnp.bfloat16)


def norm_mod(latent_stream, scale_term, offset_term):
    widened = latent_stream.astype(jnp.float32)
    average = jnp.mean(widened, axis=-1, keepdims=True)
    centred = widened - average
    spread = jnp.mean(centred * centred, axis=-1, keepdims=True)
    normed = (
        centred * lax.rsqrt(spread + 1e-06) * (1.0 + scale_term[:, None, :])
        + offset_term[:, None, :]
    )
    return normed.astype(jnp.bfloat16)


def attention(qkv_cols, log_scale, cached_keys, cached_values):
    qkv = lax.all_to_all(qkv_cols, "tp", split_axis=0, concat_axis=3, tiled=True)
    images = qkv.shape[0]
    count = qkv.shape[1]
    widened = qkv.astype(jnp.float32)
    query = widened[:, :, 0].reshape(images, count, FOCUS_GROUPS, HEAD_DIM)
    new_keys = widened[:, :, 1].reshape(images, count, FOCUS_GROUPS, HEAD_DIM)
    new_values = qkv[:, :, 2].reshape(images, count, FOCUS_GROUPS, HEAD_DIM)
    head_mult = jnp.exp(jnp.minimum(log_scale, LOG_CAP))
    query = (
        query
        * lax.rsqrt(jnp.sum(query * query, axis=-1, keepdims=True) + 1e-06)
        * head_mult[:, None]
    )
    new_keys = new_keys * lax.rsqrt(jnp.sum(new_keys * new_keys, axis=-1, keepdims=True) + 1e-06)
    all_keys = jnp.concatenate(
        [cached_keys.astype(jnp.float32).reshape(images, -1, FOCUS_GROUPS, HEAD_DIM), new_keys],
        axis=1,
    )
    all_values = jnp.concatenate(
        [cached_values.reshape(images, -1, FOCUS_GROUPS, HEAD_DIM), new_values], axis=1
    )
    scores = jnp.einsum("iqhd,ikhd->ihqk", query, all_keys, precision=lax.Precision.HIGHEST)
    maximum = jnp.max(scores, axis=-1, keepdims=True)
    weights = jnp.exp(scores - maximum)
    probabilities = (weights / jnp.sum(weights, axis=-1, keepdims=True)).astype(jnp.bfloat16)
    mixed = jnp.einsum(
        "ihqk,ikhd->iqhd", probabilities, all_values, preferred_element_type=jnp.float32
    )
    return mixed.reshape(images, count, FOCUS_GROUPS * HEAD_DIM).astype(jnp.bfloat16)


def project_out(attended, out_matrix):
    return jnp.dot(
        lax.all_gather(attended, "tp", axis=0, tiled=True),
        out_matrix,
        preferred_element_type=jnp.float32,
    )


def pass_on(latent_stream):
    return shifted(latent_stream, "section", 1)


def general(
    awaiting_arrivals,
    label_numbers,
    drawn_coarse_codes,
    discrete_prototypes,
    code_raising_operator,
    placement_tier_features,
    label_feature_rows,
    conditioned_gain_mapping,
    conditioned_shift_addend,
    question_answer_operator,
    mixing_return_operator,
    focus_sharpness_exponents,
    prior_resolution_probes,
    prior_resolution_answers,
):
    sections = lax.axis_size("section")
    section_at = lax.axis_index("section")
    group_index = lax.axis_index("tp")
    moments = prior_resolution_probes.shape[1]
    width = question_answer_operator.shape[1]
    column_width = question_answer_operator.shape[3]
    images = drawn_coarse_codes.shape[1]
    resident_pictures = awaiting_arrivals.shape[1]
    class_rows = lax.dynamic_slice_in_dim(label_numbers, sections - 1 - section_at, moments, 0)
    class_part = jnp.take(label_feature_rows, class_rows, axis=0)
    activated_part = jax.nn.silu(class_part.astype(jnp.float32)).astype(jnp.bfloat16)
    gated_response = lax.all_gather(activated_part, "tp", axis=2, tiled=True)
    flat_active = gated_response.reshape(moments * images, width)
    inner_block = 0
    local_mod = conditioned_gain_mapping[inner_block].reshape(width, 3 * column_width)
    modulated = jnp.dot(flat_active, local_mod, preferred_element_type=jnp.float32)
    mod_list = [
        modulated.reshape(moments, images, 3, column_width) + conditioned_shift_addend[inner_block]
    ]
    mod_cols = jnp.stack(mod_list)
    resample_table = resampler()
    emitted = []
    mod_rows = lax.all_to_all(mod_cols, "tp", split_axis=2, concat_axis=4, tiled=True)
    own_tokens = lax.dynamic_slice_in_dim(
        drawn_coarse_codes, group_index * resident_pictures, resident_pictures, 1
    )
    entering = embed(
        own_tokens,
        discrete_prototypes,
        code_raising_operator,
        placement_tier_features,
        resample_table,
    )
    passed_along_activation = awaiting_arrivals[0]
    for clock_tick in range(moments):
        latent_stream = passed_along_activation
        inner_block = 0
        modulation = mod_rows[inner_block, clock_tick]
        normed = norm_mod(latent_stream, modulation[:, 1], modulation[:, 2])
        local_qkv = question_answer_operator[inner_block].reshape(width, 3 * column_width)

        def body_product(portion, offset, local_qkv=local_qkv):
            return jnp.dot(portion, local_qkv, preferred_element_type=jnp.float32).astype(
                jnp.bfloat16
            )

        qkv_cols = body_product(lax.all_gather(normed, "tp", axis=0, tiled=True), jnp.int32(0))
        qkv_cols = qkv_cols.reshape(qkv_cols.shape[0], qkv_cols.shape[1], 3, column_width)
        attended = attention(
            qkv_cols,
            focus_sharpness_exponents[inner_block],
            prior_resolution_probes[inner_block, clock_tick],
            prior_resolution_answers[inner_block, clock_tick],
        )
        projected_cols = project_out(attended, mixing_return_operator[inner_block]).astype(
            jnp.bfloat16
        )
        projected = lax.all_to_all(projected_cols, "tp", split_axis=0, concat_axis=2, tiled=True)
        latent_stream = (
            latent_stream.astype(jnp.float32)
            + modulation[:, 0][:, None, :] * projected.astype(jnp.float32)
        ).astype(jnp.bfloat16)
        emitted.append(latent_stream)
        if clock_tick + 1 < moments:
            arrived = pass_on(latent_stream)
            passed_along_activation = jnp.where(section_at == 0, entering[clock_tick], arrived)
    result = jnp.stack(emitted)
    return result[None]


SLOT = 32
F32 = jnp.float32
BF16 = jnp.bfloat16
KERNEL_VMEM = 16 * 1024 * 1024


def first_head(pair, pair_width, head_dim):
    return (2 * pair * pair_width + head_dim) // (2 * head_dim)


class Plan:
    def __init__(self, section, tp, args):
        (arrivals, _, codes, prototypes, _, placement, labels, gain, _, _, _, sharp, probes, _) = args
        self.section, self.tp = section, tp
        self.pairs = tp // 2
        self.width = gain.shape[1]
        self.cols = gain.shape[3]
        self.pair_cols = 2 * self.cols
        self.heads = sharp.shape[1]
        self.head_dim = self.width // self.heads
        self.tokens = placement.shape[0]
        self.ctx = probes.shape[3]
        self.ticks = probes.shape[1]
        self.images = codes.shape[1]
        self.resident = arrivals.shape[1]
        self.used = self.pairs * self.tokens
        self.dense = self.used + -self.used % 8
        self.lanes = self.pairs * SLOT
        self.classes = labels.shape[0]
        self.vocab, self.code_dim = prototypes.shape
        starts = [first_head(p, self.pair_cols, self.head_dim) for p in range(self.pairs + 1)]
        self.starts = starts
        self.counts = [starts[p + 1] - starts[p] for p in range(self.pairs)]
        self.most = max(self.counts)
        self.left = [p * self.pair_cols - starts[p] * self.head_dim for p in range(self.pairs)]
        self.need = [
            max(0, starts[p + 1] * self.head_dim - (p + 1) * self.pair_cols)
            for p in range(self.pairs)
        ]
        self.halo = max(self.need)
        self.rows = max(self.pair_cols + self.halo, self.most * self.head_dim - min(self.left))
        self.fits = (
            tp % 2 == 0
            and self.pairs & (self.pairs - 1) == 0
            and gain.shape[0] == 1
            and codes.shape[0] == 1
            and self.ticks == 2
            and self.resident == 1
            and self.images == tp
            and self.cols % 16 == 0
            and self.head_dim == HEAD_DIM
            and starts[-1] == self.heads
            and max(self.left) <= 0
            and all(offset % 16 == 0 for offset in self.left)
            and 0 < self.halo <= self.cols
            and self.halo % 16 == 0
            and self.tokens <= SLOT
            and self.ctx <= SLOT
            and self.lanes == 128
        )


def dot(left, right, contract=((1,), (0,)), precision=None):
    return lax.dot_general(
        left, right, (contract, ((), ())), preferred_element_type=F32, precision=precision
    )


def image_of(token, plan):
    image = jnp.zeros(token.shape, jnp.int32)
    for at in range(1, plan.pairs + 1):
        image += (token >= at * plan.tokens).astype(jnp.int32)
    return image


def spread(rows, tick, plan):
    part = rows[tick * plan.pairs : (tick + 1) * plan.pairs, :]
    parts = []
    for _ in range(3):
        rounded = part.astype(BF16).astype(F32)
        parts.append(rounded)
        part = part - rounded
    count = 3 * plan.pairs
    stacked = jnp.concatenate(parts, axis=0).astype(BF16)
    row = lax.broadcasted_iota(jnp.int32, (count, plan.lanes), 0)
    lane = lax.broadcasted_iota(jnp.int32, (count, plan.lanes), 1)
    pick = (row % plan.pairs == image_of(lane, plan)).astype(F32).astype(BF16)
    return dot(stacked, pick, ((0,), (0,)))


def modulation_kernel(plan, *refs):
    pairs = plan.pairs
    near, far = refs[:pairs], refs[pairs : 2 * pairs]
    matrix, addend, shift, gate, active = refs[2 * pairs :]
    place = lax.axis_index("tp")
    core, pair = place % 2, place // 2
    rows = plan.ticks * plan.images
    for k in range(pairs):
        for side, piece in enumerate((near[k], far[k])):
            value = piece[...].astype(F32)
            value = jnp.concatenate([value, jnp.zeros((128 - rows, plan.cols), F32)], axis=0).T
            start = (pair ^ k) * plan.pair_cols + (core if side == 0 else 1 - core) * plan.cols
            active[pl.ds(pl.multiple_of(start, 16), plan.cols), :] = value.astype(BF16)
    tokens = active[...]
    for part in range(3):
        value = dot(matrix[part], tokens).T[:rows] + addend[part]
        if part:
            shift[part - 1] = value
        else:
            gate[...] = value


def opening_kernel(
    plan, labels, table, arrival, probes, answers, matrix, gain, active, edge, gained, *outs
):
    *outs, picked, arrived = outs
    halo = pltpu.make_async_copy(matrix.at[:, : plan.halo, :], edge, arrived.at[0])
    halo.start()
    fetch = pltpu.make_async_copy(gain, gained, arrived.at[1])
    fetch.start()
    pairs = plan.pairs
    pair = lax.axis_index("tp") // 2
    section_at = lax.axis_index("section")
    place = lax.broadcasted_iota(jnp.int32, (1, plan.classes), 1)
    row = 0
    for core in range(2):
        for tick in range(plan.ticks):
            for other in range(pairs):
                label = labels[tick - section_at + plan.section - 1, 2 * other + core]
                picked[row : row + 1, :] = (place == label).astype(F32)
                row += 1
    value = dot(picked[...].astype(BF16), table[...], ((1,), (1,)))
    active[...] = (value / (1.0 + jnp.exp(-value))).astype(BF16)

    span = plan.most * plan.head_dim
    first, stores = outs[0], outs[1:]
    wide = arrival[...].astype(F32)
    chunks = []
    for at in range(pairs):
        chunk = wide[:, at * plan.pair_cols : (at + 1) * plan.pair_cols]
        chunks.append(
            jnp.concatenate([chunk, jnp.zeros((plan.tokens, span - plan.pair_cols), F32)], axis=1)
        )
    first[...] = jnp.concatenate(
        chunks + [jnp.zeros((first.shape[0] - pairs * plan.tokens, span), F32)], axis=0
    ).astype(BF16)

    for source, stored in enumerate((probes, answers)):
        full = stored[...].astype(F32)
        for tick in range(plan.ticks):
            value = full[:, tick, :]
            for at in range(pairs):
                start = plan.starts[at] * plan.head_dim
                reach = min(span, plan.width - start)
                part = value[:, start : start + reach]
                if reach < span:
                    part = jnp.concatenate(
                        [part, jnp.zeros((plan.ctx, span - reach), F32)], axis=1
                    )
                part = jnp.concatenate(
                    [part, jnp.zeros((SLOT - plan.ctx, span), F32)], axis=0
                ).astype(BF16)
                for k in range(pairs):

                    @pl.when((pair ^ k) == at)
                    def _(k=k, part=part, tick=tick, source=source):
                        stores[tick * pairs + k][source] = part

    halo.wait()
    fetch.wait()


def embed_kernel(plan, codes, table, resample, raising, placement, out):
    place = lax.axis_index("tp")
    core, pair = place % 2, place // 2
    row = lax.broadcasted_iota(jnp.int32, (plan.vocab, plan.lanes), 0)
    blank = jnp.zeros((1, SLOT - plan.ctx), jnp.int32)
    slots = []
    for image in range(plan.pairs):
        both = codes[2 * image : 2 * image + 2, :]
        slots += [jnp.where(core == 0, both[:1], both[1:]), blank]
    picked = (row == jnp.concatenate(slots, axis=1)).astype(F32)
    looked = dot(table[...], picked, precision=lax.Precision.HIGHEST)
    mapped = dot(looked, resample[...], precision=lax.Precision.HIGHEST).astype(BF16)
    fixed = jnp.concatenate(
        [placement[...].astype(F32)] * plan.pairs
        + [jnp.zeros((plan.lanes - plan.used, plan.width), F32)],
        axis=0,
    )
    full = (dot(mapped, raising[...], ((0,), (0,))) + fixed)[: plan.dense].astype(BF16)
    for at in range(plan.pairs):

        @pl.when(pair == at)
        def _(at=at):
            out[...] = full[:, at * plan.pair_cols : (at + 1) * plan.pair_cols]


def project(plan, tick, pieces, shifts, weights, held, qkv, wide, scale_at, offset_at, turning):
    pairs = plan.pairs
    mine, other, near, far = weights
    half = plan.ticks * plan.pairs
    place = lax.axis_index("tp")
    core, pair = place % 2, place // 2
    cols, pair_cols, lanes = plan.cols, plan.pair_cols, plan.lanes
    turning[plan.used :, :] = jnp.zeros((lanes - plan.used, plan.width), F32)
    for k in range(pairs):
        at = pair ^ k
        piece = pieces[k][...].astype(F32)
        if tick == 0:
            chunks = [
                piece[j * plan.tokens : (j + 1) * plan.tokens, :pair_cols] for j in range(pairs)
            ]
            piece = jnp.concatenate(chunks, axis=1)
        for place_at in range(pairs):

            @pl.when(at == place_at)
            def _(place_at=place_at, piece=piece):
                if tick:
                    span = slice(place_at * pair_cols, (place_at + 1) * pair_cols)
                    turning[: plan.used, span] = piece[: plan.used]
                else:
                    turning[place_at * plan.tokens : (place_at + 1) * plan.tokens, :] = piece

        for side in range(2):
            start = pl.multiple_of(
                at * pair_cols + (core if side == 0 else 1 - core) * cols, 16
            )
            own = pl.ds(pl.multiple_of(core * half, 8), half)
            scale_at[pl.ds(start, cols), :] = spread(shifts[side][k][0, own, :], tick, plan)
            offset_at[pl.ds(start, cols), :] = spread(shifts[side][k][1, own, :], tick, plan)
    value = turning[...].T
    wide[...] = value
    average = jnp.sum(value, axis=0, keepdims=True) * (1.0 / plan.width)
    centred = value - average
    variance = jnp.sum(centred * centred, axis=0, keepdims=True) * (1.0 / plan.width)
    result = centred * lax.rsqrt(variance + 1e-06) * (1.0 + scale_at[...]) + offset_at[...]
    tokens = result.astype(BF16)
    start = pl.multiple_of(pair * pair_cols, 16)
    held[...] = wide[pl.ds(start, pair_cols), :].astype(BF16)
    if plan.rows > pair_cols + plan.halo:
        qkv[:, pair_cols + plan.halo :, :] = jnp.zeros(
            (3, plan.rows - pair_cols - plan.halo, lanes), BF16
        )
    for part in range(3):
        start = pl.multiple_of(core * cols, 16)
        qkv[part, pl.ds(start, cols), :] = dot(mine[part], tokens).astype(BF16)
        start = pl.multiple_of((1 - core) * cols, 16)
        qkv[part, pl.ds(start, cols), :] = dot(other[part], tokens).astype(BF16)
        edge = jnp.where(core == 1, near[part].astype(F32), far[part].astype(F32)).astype(BF16)
        qkv[part, pair_cols : pair_cols + plan.halo, :] = dot(edge, tokens).astype(BF16)


def attend(plan, stores, qkv, sharp, attended, cached, mixed_at):
    pairs, pair_cols, dim, lanes = plan.pairs, plan.pair_cols, plan.head_dim, plan.lanes
    pair = lax.axis_index("tp") // 2
    for k in range(pairs):
        slot = pl.multiple_of((pair ^ k) * SLOT, SLOT)
        cached[0, pl.ds(slot, SLOT), :] = stores[k][0]
        cached[1, pl.ds(slot, SLOT), :] = stores[k][1]
    head_at = first_head(pair, pair_cols, dim)
    begin = head_at * dim - pair * pair_cols
    row = lax.broadcasted_iota(jnp.int32, (lanes, lanes), 0)
    lane = lax.broadcasted_iota(jnp.int32, (lanes, lanes), 1)
    image = image_of(lane, plan)
    old_ok = (row // SLOT == image) & (row % SLOT < plan.ctx)
    new_ok = (image_of(row, plan) == image) & (row < plan.used)
    queries, keys, values, lifts, key_scales = [], [], [], [], []
    for head in range(plan.most):
        at = pl.ds(pl.multiple_of(begin + head * dim, 16), dim)
        query, key, value = qkv[0, at, :], qkv[1, at, :], qkv[2, at, :]
        wide_query, wide_key = query.astype(F32), key.astype(F32)
        lift = sharp[0, jnp.minimum(head_at + head, plan.heads - 1)]
        lift = jnp.exp(jnp.minimum(jnp.full((1, lanes), lift, F32), LOG_CAP))
        lifts.append(
            lax.rsqrt(jnp.sum(wide_query * wide_query, axis=0, keepdims=True) + 1e-06) * lift
        )
        key_scales.append(lax.rsqrt(jnp.sum(wide_key * wide_key, axis=0, keepdims=True) + 1e-06))
        queries.append(query)
        keys.append(key)
        values.append(value)
    pad = -plan.most % 8
    key_cols = jnp.concatenate(
        key_scales + ([jnp.zeros((pad, lanes), F32)] if pad else []), axis=0
    ).T
    old_keys, old_values = cached[0], cached[1]
    for head in range(plan.most):
        span = slice(head * dim, (head + 1) * dim)
        old = dot(old_keys[:, span], queries[head]) * lifts[head]
        new = (
            dot(keys[head], queries[head], ((0,), (0,)))
            * key_cols[:, head : head + 1]
            * lifts[head]
        )
        old = jnp.where(old_ok, old, -1e30)
        new = jnp.where(new_ok, new, -1e30)
        top = jnp.maximum(
            jnp.max(old, axis=0, keepdims=True), jnp.max(new, axis=0, keepdims=True)
        )
        old, new = jnp.exp(old - top), jnp.exp(new - top)
        total = 1.0 / (jnp.sum(old, axis=0, keepdims=True) + jnp.sum(new, axis=0, keepdims=True))
        old, new = (old * total).astype(BF16), (new * total).astype(BF16)
        mixed = dot(old_values[:, span], old, ((0,), (0,))) + dot(values[head], new)
        mixed_at[head * dim : (head + 1) * dim, :] = mixed
    attended[...] = mixed_at[...].T[: plan.dense].astype(BF16)


def project_kernel(plan, tick, *refs):
    pairs = plan.pairs
    project(
        plan,
        tick,
        refs[:pairs],
        (refs[pairs : 2 * pairs], refs[2 * pairs : 3 * pairs]),
        refs[3 * pairs : 3 * pairs + 4],
        *refs[3 * pairs + 4 :],
    )


def attend_kernel(plan, *refs):
    attend(plan, refs[: plan.pairs], *refs[plan.pairs :])


def layer_kernel(plan, tick, *refs):
    pairs = plan.pairs
    attended, held, cached, mixed_at, qkv, *rest = refs[4 * pairs + 5 :]
    project(
        plan,
        tick,
        refs[:pairs],
        (refs[pairs : 2 * pairs], refs[2 * pairs : 3 * pairs]),
        refs[4 * pairs : 4 * pairs + 4],
        held,
        qkv,
        *rest,
    )
    attend(plan, refs[3 * pairs : 4 * pairs], qkv, refs[4 * pairs + 4], attended, cached, mixed_at)


def return_kernel(plan, tick, *refs):
    pairs = plan.pairs
    pieces = refs[:pairs]
    mine, other, held, gate_mine, gate_other = refs[pairs : pairs + 5]
    rest = refs[pairs + 5 :]
    if tick == 0:
        entering, onward, *rows = rest[:-3]
    else:
        rows = rest[:-3]
    joined, projected, gate = rest[-3:]
    place = lax.axis_index("tp")
    core, pair = place % 2, place // 2
    cols, dim = plan.cols, plan.head_dim
    half = plan.ticks * pairs
    joined[plan.used :, :] = jnp.zeros((plan.lanes - plan.used, plan.width), BF16)
    for k in range(pairs):
        for at in range(pairs):

            @pl.when((pair ^ k) == at)
            def _(k=k, at=at):
                start, count = plan.starts[at] * dim, plan.counts[at] * dim
                joined[: plan.dense, start : start + count] = pieces[k][:, :count]

    value = joined[...]
    for side, (matrix, gates) in enumerate(((mine, gate_mine), (other, gate_other))):
        start = pl.multiple_of((core if side == 0 else 1 - core) * cols, 16)
        projected[pl.ds(start, cols), :] = dot(matrix[...], value, ((1,), (1,))).astype(BF16).astype(F32)
        gates = gates[pl.ds(pl.multiple_of(core * half, 8), half), :]
        gate[pl.ds(start, cols), :] = spread(gates, tick, plan)
    result = held[...].astype(F32) + gate[...] * projected[...]
    turned = result.T
    for k in range(pairs):
        for image in range(pairs):

            @pl.when((pair ^ k) == image)
            def _(k=k, image=image):
                rows[k][...] = turned[image * plan.tokens : (image + 1) * plan.tokens, :].astype(BF16)

    if tick == 0:
        last = lax.axis_index("section") == plan.section - 1
        onward[...] = jnp.where(last, entering[...].astype(F32), turned[: plan.dense]).astype(BF16)


def gather_kernel(plan, *refs):
    pairs = plan.pairs
    pieces, out, full = refs[:-2], refs[-2], refs[-1]
    pair = lax.axis_index("tp") // 2
    for tick in range(plan.ticks):
        for k in range(pairs):
            for at in range(pairs):

                @pl.when((pair ^ k) == at)
                def _(tick=tick, k=k, at=at):
                    full[tick, :, at * plan.pair_cols : (at + 1) * plan.pair_cols] = pieces[
                        tick * pairs + k
                    ][...].astype(F32)

    out[...] = jnp.stack([full[tick] for tick in range(plan.ticks)], axis=1).astype(BF16)


def resample_blocks(plan):
    blocks = []
    for coarse in range(1, SIDE):
        fine = np.arange(SIDE, dtype=np.float32)
        rough = np.arange(coarse, dtype=np.float32)
        one = np.float32(1.0)
        size, parts = np.float32(SIDE), np.float32(coarse)
        begins = np.maximum(fine[:, None] / size, rough[None, :] / parts)
        finish = np.minimum((fine[:, None] + one) / size, (rough[None, :] + one) / parts)
        crossing = np.maximum(finish - begins, np.float32(0.0)) * size
        blocks.append(
            (crossing[:, None, :, None] * crossing[None, :, None, :]).reshape(
                SIDE * SIDE, coarse * coarse
            )
        )
    table = np.concatenate(blocks, axis=1).astype(np.float32)
    full = np.zeros((plan.lanes, plan.lanes), np.float32)
    for image in range(plan.pairs):
        at = image * SLOT
        to = image * plan.tokens
        full[at : at + table.shape[1], to : to + table.shape[0]] = table.T
    return full


def paired(plan, *args):
    (
        awaiting_arrivals,
        label_numbers,
        drawn_coarse_codes,
        discrete_prototypes,
        code_raising_operator,
        placement_tier_features,
        label_feature_rows,
        conditioned_gain_mapping,
        conditioned_shift_addend,
        question_answer_operator,
        mixing_return_operator,
        focus_sharpness_exponents,
        prior_resolution_probes,
        prior_resolution_answers,
    ) = args
    pairs, tp, cols, pair_cols = plan.pairs, plan.tp, plan.cols, plan.pair_cols
    width, lanes, dim, ticks = plan.width, plan.lanes, plan.head_dim, plan.ticks
    rows = ticks * plan.images

    def swap(value, k):
        return lax.ppermute(value, "tp", [(g, g ^ (2 * k)) for g in range(tp)])

    def across(value):
        return lax.ppermute(value, "tp", [(g, g ^ 1) for g in range(tp)])

    def around(value):
        return [value] + [swap(value, k) for k in range(1, pairs)]

    def call(kernel, outs, scratch, values, scalars=(), loose=(), raw=(), space=pltpu.VMEM):
        ins = [
            pltpu.with_memory_space_constraint(
                v, pltpu.HBM if i in (*scalars, *loose, *raw) else pltpu.VMEM
            )
            for i, v in enumerate(values)
        ]
        return pl.pallas_call(
            lambda *refs: kernel(plan, *refs),
            out_shape=[space(shape, dtype) for shape, dtype in outs],
            in_specs=[
                pl.BlockSpec(
                    memory_space=pltpu.SMEM
                    if i in scalars
                    else pl.ANY
                    if i in raw
                    else pltpu.VMEM
                )
                for i in range(len(values))
            ],
            out_specs=[pl.BlockSpec(memory_space=pltpu.VMEM)] * len(outs),
            scratch_shapes=scratch,
            compiler_params=pltpu.CompilerParams(vmem_limit_bytes=KERNEL_VMEM),
        )(*ins)

    span = plan.most * dim
    qkv_mine = jnp.transpose(question_answer_operator[0], (1, 2, 0))
    active, edge, mod_matrix, first, *stores = call(
        opening_kernel,
        [
            ((rows, cols), BF16),
            ((3, plan.halo, width), BF16),
            ((3, cols, width), BF16),
            ((plan.dense, span), BF16),
        ]
        + [((2, SLOT, span), BF16)] * (ticks * pairs),
        [pltpu.VMEM((rows, plan.classes), F32), pltpu.SemaphoreType.DMA((2,))],
        [
            label_numbers,
            label_feature_rows.T,
            awaiting_arrivals[0, 0],
            jnp.transpose(prior_resolution_probes[0, :, 0], (1, 0, 2)),
            jnp.transpose(prior_resolution_answers[0, :, 0], (1, 0, 2)),
            qkv_mine,
            jnp.transpose(conditioned_gain_mapping[0], (1, 2, 0)),
        ],
        (0,),
        (1, 2, 3, 4),
        (5, 6),
    )
    active = around(active)
    active += [across(piece) for piece in active]
    shift, gate = call(
        modulation_kernel,
        [((2, rows, cols), F32), ((rows, cols), F32)],
        [pltpu.VMEM((width, 128), BF16)],
        [
            *active,
            mod_matrix,
            jnp.transpose(conditioned_shift_addend, (1, 0, 2)),
        ],
    )
    shifts = around(shift)
    shifts += [across(piece) for piece in shifts]
    gate_back = across(gate)

    qkv_other = across(qkv_mine)
    out_mine = mixing_return_operator[0].T
    out_other = across(out_mine)
    near = lax.ppermute(edge, "tp", [(2 * p + 2, 2 * p + 1) for p in range(pairs) if plan.need[p]])
    far = across(near)
    pieces = around(first)
    cached = [
        [stores[tick * pairs]]
        + [swap(stores[tick * pairs + k], k) for k in range(1, pairs)]
        for tick in range(ticks)
    ]
    (entering,) = call(
        embed_kernel,
        [((plan.dense, pair_cols), BF16)],
        [],
        [
            drawn_coarse_codes[0],
            discrete_prototypes.T,
            jnp.asarray(resample_blocks(plan)),
            code_raising_operator,
            placement_tier_features,
        ],
    )

    emitted = []
    for tick in range(ticks):
        wide = [pltpu.VMEM((width, lanes), F32)] * 3 + [pltpu.VMEM((lanes, width), F32)]
        heads_of = [pltpu.VMEM((2, lanes, span), BF16), pltpu.VMEM((span, lanes), F32)]
        weights = [qkv_mine, qkv_other, near, far]
        if tick == 0:
            held, qkv = call(
                lambda *refs: project_kernel(refs[0], 0, *refs[1:]),
                [((pair_cols, lanes), BF16), ((3, plan.rows, lanes), BF16)],
                wide,
                [*pieces, *shifts, *weights],
            )
            (attended,) = call(
                attend_kernel,
                [((plan.dense, span), BF16)],
                heads_of,
                [*cached[tick], qkv, focus_sharpness_exponents],
                (pairs + 1,),
            )
        else:
            values = [*pieces, *shifts, *cached[tick], *weights, focus_sharpness_exponents]
            attended, held = call(
                lambda *refs, tick=tick: layer_kernel(refs[0], tick, *refs[1:]),
                [((plan.dense, span), BF16), ((pair_cols, lanes), BF16)],
                heads_of + [pltpu.VMEM((3, plan.rows, lanes), BF16)] + wide,
                values,
                (len(values) - 1,),
            )
        outs = [((plan.tokens, pair_cols), BF16)] * pairs
        extra = []
        if tick + 1 < ticks:
            outs = [((plan.dense, pair_cols), BF16)] + outs
            extra = [entering]
        results = call(
            lambda *refs, tick=tick: return_kernel(refs[0], tick, *refs[1:]),
            outs,
            [
                pltpu.VMEM((lanes, width), BF16),
                pltpu.VMEM((pair_cols, lanes), F32),
                pltpu.VMEM((pair_cols, lanes), F32),
            ],
            [
                *around(attended),
                out_mine,
                out_other,
                held,
                gate,
                gate_back,
                *extra,
            ],
        )
        if tick + 1 < ticks:
            onward = lax.ppermute(
                results[0],
                "section",
                [(s, (s + 1) % plan.section) for s in range(plan.section)],
            )
            pieces = around(onward)
        final = results[-pairs:]
        emitted += [final[0]] + [swap(final[k], k) for k in range(1, pairs)]
    (out,) = call(
        gather_kernel,
        [((plan.tokens, ticks, width), BF16)],
        [pltpu.VMEM((ticks, plan.tokens, width), F32)],
        emitted,
        space=pltpu.HBM,
    )
    return jnp.transpose(out, (1, 0, 2))[None, :, None]


def local(*args):
    plan = Plan(lax.axis_size("section"), lax.axis_size("tp"), args)
    return paired(plan, *args) if plan.fits else general(*args)


def solution(mesh):
    in_specs = (
        P("section", "tp", None, None),
        P(),
        P(),
        P(),
        P(),
        P(),
        P(None, "tp"),
        P("section", None, None, "tp"),
        P("section", None, "tp"),
        P("section", None, None, "tp"),
        P("section", None, "tp"),
        P("section", None),
        P("section", None, "tp", None, None),
        P("section", None, "tp", None, None),
    )
    out_specs = P("section", None, "tp", None, None)
    return jax.shard_map(local, mesh=mesh, in_specs=in_specs, out_specs=out_specs, check_vma=False)
```

```python
import jax
import jax.numpy as jnp
from jax import lax
from jax.experimental import pallas as pl
from jax.experimental.pallas import tpu as pltpu
from jax.sharding import PartitionSpec as P
import numpy as np

FOCUS_GROUPS = 30
HEAD_DIM = 64
SIDE = 5


LOG_CAP = 4.605170185988092


def shifted(value, axis, steps):
    count = lax.axis_size(axis)
    first, last = (max(0, -steps), min(count, count - steps))
    return lax.ppermute(value, axis, [(source, source + steps) for source in range(first, last)])


def crossing_matrix(target, coarse):
    fine_index = jnp.arange(target, dtype=jnp.float32)
    coarse_index = jnp.arange(coarse, dtype=jnp.float32)
    begins = jnp.maximum(fine_index[:, None] / target, coarse_index[None, :] / coarse)
    finish = jnp.minimum(
        (fine_index[:, None] + 1.0) / target, (coarse_index[None, :] + 1.0) / coarse
    )
    return jnp.maximum(finish - begins, 0.0) * target


def resampler():
    blocks = []
    for coarse in range(1, SIDE):
        crossing = crossing_matrix(SIDE, coarse)
        blocks.append(
            (crossing[:, None, :, None] * crossing[None, :, None, :]).reshape(
                SIDE * SIDE, coarse * coarse
            )
        )
    return jnp.concatenate(blocks, axis=1)


def embed(
    drawn_coarse_codes,
    discrete_prototypes,
    code_raising_operator,
    placement_tier_features,
    resample_table,
):
    looked_up = discrete_prototypes[drawn_coarse_codes]
    mapped = jnp.einsum(
        "tc,nicv->nitv", resample_table, looked_up, precision=lax.Precision.HIGHEST
    ).astype(jnp.bfloat16)
    leading = mapped.shape[:3]
    projected_rows = jnp.dot(
        mapped.reshape(-1, mapped.shape[3]),
        code_raising_operator,
        preferred_element_type=jnp.float32,
    )
    projected_rows = projected_rows.reshape(leading + (code_raising_operator.shape[1],))
    return (projected_rows + placement_tier_features.astype(jnp.float32)).astype(jnp.bfloat16)


def norm_mod(latent_stream, scale_term, offset_term):
    widened = latent_stream.astype(jnp.float32)
    average = jnp.mean(widened, axis=-1, keepdims=True)
    centred = widened - average
    spread = jnp.mean(centred * centred, axis=-1, keepdims=True)
    normed = (
        centred * lax.rsqrt(spread + 1e-06) * (1.0 + scale_term[:, None, :])
        + offset_term[:, None, :]
    )
    return normed.astype(jnp.bfloat16)


def attention(qkv_cols, log_scale, cached_keys, cached_values):
    qkv = lax.all_to_all(qkv_cols, "tp", split_axis=0, concat_axis=3, tiled=True)
    images = qkv.shape[0]
    count = qkv.shape[1]
    widened = qkv.astype(jnp.float32)
    query = widened[:, :, 0].reshape(images, count, FOCUS_GROUPS, HEAD_DIM)
    new_keys = widened[:, :, 1].reshape(images, count, FOCUS_GROUPS, HEAD_DIM)
    new_values = qkv[:, :, 2].reshape(images, count, FOCUS_GROUPS, HEAD_DIM)
    head_mult = jnp.exp(jnp.minimum(log_scale, LOG_CAP))
    query = (
        query
        * lax.rsqrt(jnp.sum(query * query, axis=-1, keepdims=True) + 1e-06)
        * head_mult[:, None]
    )
    new_keys = new_keys * lax.rsqrt(jnp.sum(new_keys * new_keys, axis=-1, keepdims=True) + 1e-06)
    all_keys = jnp.concatenate(
        [cached_keys.astype(jnp.float32).reshape(images, -1, FOCUS_GROUPS, HEAD_DIM), new_keys],
        axis=1,
    )
    all_values = jnp.concatenate(
        [cached_values.reshape(images, -1, FOCUS_GROUPS, HEAD_DIM), new_values], axis=1
    )
    scores = jnp.einsum("iqhd,ikhd->ihqk", query, all_keys, precision=lax.Precision.HIGHEST)
    maximum = jnp.max(scores, axis=-1, keepdims=True)
    weights = jnp.exp(scores - maximum)
    probabilities = (weights / jnp.sum(weights, axis=-1, keepdims=True)).astype(jnp.bfloat16)
    mixed = jnp.einsum(
        "ihqk,ikhd->iqhd", probabilities, all_values, preferred_element_type=jnp.float32
    )
    return mixed.reshape(images, count, FOCUS_GROUPS * HEAD_DIM).astype(jnp.bfloat16)


def project_out(attended, out_matrix):
    return jnp.dot(
        lax.all_gather(attended, "tp", axis=0, tiled=True),
        out_matrix,
        preferred_element_type=jnp.float32,
    )


def pass_on(latent_stream):
    return shifted(latent_stream, "section", 1)


def general(
    awaiting_arrivals,
    label_numbers,
    drawn_coarse_codes,
    discrete_prototypes,
    code_raising_operator,
    placement_tier_features,
    label_feature_rows,
    conditioned_gain_mapping,
    conditioned_shift_addend,
    question_answer_operator,
    mixing_return_operator,
    focus_sharpness_exponents,
    prior_resolution_probes,
    prior_resolution_answers,
):
    sections = lax.axis_size("section")
    section_at = lax.axis_index("section")
    group_index = lax.axis_index("tp")
    moments = prior_resolution_probes.shape[1]
    width = question_answer_operator.shape[1]
    column_width = question_answer_operator.shape[3]
    images = drawn_coarse_codes.shape[1]
    resident_pictures = awaiting_arrivals.shape[1]
    class_rows = lax.dynamic_slice_in_dim(label_numbers, sections - 1 - section_at, moments, 0)
    class_part = jnp.take(label_feature_rows, class_rows, axis=0)
    activated_part = jax.nn.silu(class_part.astype(jnp.float32)).astype(jnp.bfloat16)
    gated_response = lax.all_gather(activated_part, "tp", axis=2, tiled=True)
    flat_active = gated_response.reshape(moments * images, width)
    inner_block = 0
    local_mod = conditioned_gain_mapping[inner_block].reshape(width, 3 * column_width)
    modulated = jnp.dot(flat_active, local_mod, preferred_element_type=jnp.float32)
    mod_list = [
        modulated.reshape(moments, images, 3, column_width) + conditioned_shift_addend[inner_block]
    ]
    mod_cols = jnp.stack(mod_list)
    resample_table = resampler()
    emitted = []
    mod_rows = lax.all_to_all(mod_cols, "tp", split_axis=2, concat_axis=4, tiled=True)
    own_tokens = lax.dynamic_slice_in_dim(
        drawn_coarse_codes, group_index * resident_pictures, resident_pictures, 1
    )
    entering = embed(
        own_tokens,
        discrete_prototypes,
        code_raising_operator,
        placement_tier_features,
        resample_table,
    )
    passed_along_activation = awaiting_arrivals[0]
    for clock_tick in range(moments):
        latent_stream = passed_along_activation
        inner_block = 0
        modulation = mod_rows[inner_block, clock_tick]
        normed = norm_mod(latent_stream, modulation[:, 1], modulation[:, 2])
        local_qkv = question_answer_operator[inner_block].reshape(width, 3 * column_width)

        def body_product(portion, offset, local_qkv=local_qkv):
            return jnp.dot(portion, local_qkv, preferred_element_type=jnp.float32).astype(
                jnp.bfloat16
            )

        qkv_cols = body_product(lax.all_gather(normed, "tp", axis=0, tiled=True), jnp.int32(0))
        qkv_cols = qkv_cols.reshape(qkv_cols.shape[0], qkv_cols.shape[1], 3, column_width)
        attended = attention(
            qkv_cols,
            focus_sharpness_exponents[inner_block],
            prior_resolution_probes[inner_block, clock_tick],
            prior_resolution_answers[inner_block, clock_tick],
        )
        projected_cols = project_out(attended, mixing_return_operator[inner_block]).astype(
            jnp.bfloat16
        )
        projected = lax.all_to_all(projected_cols, "tp", split_axis=0, concat_axis=2, tiled=True)
        latent_stream = (
            latent_stream.astype(jnp.float32)
            + modulation[:, 0][:, None, :] * projected.astype(jnp.float32)
        ).astype(jnp.bfloat16)
        emitted.append(latent_stream)
        if clock_tick + 1 < moments:
            arrived = pass_on(latent_stream)
            passed_along_activation = jnp.where(section_at == 0, entering[clock_tick], arrived)
    result = jnp.stack(emitted)
    return result[None]


SLOT = 32
F32 = jnp.float32
BF16 = jnp.bfloat16
KERNEL_VMEM = 16 * 1024 * 1024


def first_head(pair, pair_width, head_dim):
    return (2 * pair * pair_width + head_dim) // (2 * head_dim)


class Plan:
    def __init__(self, section, tp, args):
        (arrivals, _, codes, prototypes, _, placement, labels, gain, _, _, _, sharp, probes, _) = args
        self.section, self.tp = section, tp
        self.pairs = tp // 2
        self.width = gain.shape[1]
        self.cols = gain.shape[3]
        self.pair_cols = 2 * self.cols
        self.heads = sharp.shape[1]
        self.head_dim = self.width // self.heads
        self.tokens = placement.shape[0]
        self.ctx = probes.shape[3]
        self.ticks = probes.shape[1]
        self.images = codes.shape[1]
        self.resident = arrivals.shape[1]
        self.used = self.pairs * self.tokens
        self.dense = self.used + -self.used % 8
        self.lanes = self.pairs * SLOT
        self.classes = labels.shape[0]
        self.vocab, self.code_dim = prototypes.shape
        starts = [first_head(p, self.pair_cols, self.head_dim) for p in range(self.pairs + 1)]
        self.starts = starts
        self.counts = [starts[p + 1] - starts[p] for p in range(self.pairs)]
        self.most = max(self.counts)
        self.left = [p * self.pair_cols - starts[p] * self.head_dim for p in range(self.pairs)]
        self.need = [
            max(0, starts[p + 1] * self.head_dim - (p + 1) * self.pair_cols)
            for p in range(self.pairs)
        ]
        self.halo = max(self.need)
        self.rows = max(self.pair_cols + self.halo, self.most * self.head_dim - min(self.left))
        self.fits = (
            tp % 2 == 0
            and self.pairs & (self.pairs - 1) == 0
            and gain.shape[0] == 1
            and codes.shape[0] == 1
            and self.ticks == 2
            and self.resident == 1
            and self.images == tp
            and self.cols % 16 == 0
            and self.head_dim == HEAD_DIM
            and starts[-1] == self.heads
            and max(self.left) <= 0
            and all(offset % 16 == 0 for offset in self.left)
            and 0 < self.halo <= self.cols
            and self.halo % 16 == 0
            and self.tokens <= SLOT
            and self.ctx <= SLOT
            and self.lanes == 128
        )


def dot(left, right, contract=((1,), (0,)), precision=None):
    return lax.dot_general(
        left, right, (contract, ((), ())), preferred_element_type=F32, precision=precision
    )


def image_of(token, plan):
    image = jnp.zeros(token.shape, jnp.int32)
    for at in range(1, plan.pairs + 1):
        image += (token >= at * plan.tokens).astype(jnp.int32)
    return image


def spread(rows, tick, plan):
    part = rows[tick * plan.pairs : (tick + 1) * plan.pairs, :]
    parts = []
    for _ in range(3):
        rounded = part.astype(BF16).astype(F32)
        parts.append(rounded)
        part = part - rounded
    count = 3 * plan.pairs
    stacked = jnp.concatenate(parts, axis=0).astype(BF16)
    row = lax.broadcasted_iota(jnp.int32, (count, plan.lanes), 0)
    lane = lax.broadcasted_iota(jnp.int32, (count, plan.lanes), 1)
    pick = (row % plan.pairs == image_of(lane, plan)).astype(F32).astype(BF16)
    return dot(stacked, pick, ((0,), (0,)))


def modulation_kernel(plan, *refs):
    pairs = plan.pairs
    near, far = refs[:pairs], refs[pairs : 2 * pairs]
    matrix, addend, shift, gate, active = refs[2 * pairs :]
    place = lax.axis_index("tp")
    core, pair = place % 2, place // 2
    rows = plan.ticks * plan.images
    for k in range(pairs):
        for side, piece in enumerate((near[k], far[k])):
            value = piece[...].astype(F32)
            value = jnp.concatenate([value, jnp.zeros((128 - rows, plan.cols), F32)], axis=0).T
            start = (pair ^ k) * plan.pair_cols + (core if side == 0 else 1 - core) * plan.cols
            active[pl.ds(pl.multiple_of(start, 16), plan.cols), :] = value.astype(BF16)
    tokens = active[...]
    for part in range(3):
        value = dot(matrix[part], tokens).T[:rows] + addend[part]
        if part:
            shift[part - 1] = value
        else:
            gate[...] = value


def opening_kernel(
    plan, labels, table, arrival, probes, answers, matrix, gain, active, edge, gained, *outs
):
    *outs, picked, arrived = outs
    halo = pltpu.make_async_copy(matrix.at[:, : plan.halo, :], edge, arrived.at[0])
    halo.start()
    fetch = pltpu.make_async_copy(gain, gained, arrived.at[1])
    fetch.start()
    pairs = plan.pairs
    pair = lax.axis_index("tp") // 2
    section_at = lax.axis_index("section")
    place = lax.broadcasted_iota(jnp.int32, (1, plan.classes), 1)
    row = 0
    for core in range(2):
        for tick in range(plan.ticks):
            for other in range(pairs):
                label = labels[tick - section_at + plan.section - 1, 2 * other + core]
                picked[row : row + 1, :] = (place == label).astype(F32)
                row += 1
    value = dot(picked[...].astype(BF16), table[...], ((1,), (1,)))
    active[...] = (value / (1.0 + jnp.exp(-value))).astype(BF16)

    span = plan.most * plan.head_dim
    first, stores = outs[0], outs[1:]
    wide = arrival[...].astype(F32)
    chunks = []
    for at in range(pairs):
        chunk = wide[:, at * plan.pair_cols : (at + 1) * plan.pair_cols]
        chunks.append(
            jnp.concatenate([chunk, jnp.zeros((plan.tokens, span - plan.pair_cols), F32)], axis=1)
        )
    first[...] = jnp.concatenate(
        chunks + [jnp.zeros((first.shape[0] - pairs * plan.tokens, span), F32)], axis=0
    ).astype(BF16)

    for source, stored in enumerate((probes, answers)):
        full = stored[...].astype(F32)
        for tick in range(plan.ticks):
            value = full[:, tick, :]
            for at in range(pairs):
                start = plan.starts[at] * plan.head_dim
                reach = min(span, plan.width - start)
                part = value[:, start : start + reach]
                if reach < span:
                    part = jnp.concatenate(
                        [part, jnp.zeros((plan.ctx, span - reach), F32)], axis=1
                    )
                part = jnp.concatenate(
                    [part, jnp.zeros((SLOT - plan.ctx, span), F32)], axis=0
                ).astype(BF16)
                for k in range(pairs):

                    @pl.when((pair ^ k) == at)
                    def _(k=k, part=part, tick=tick, source=source):
                        stores[k][2 * tick + source] = part

    halo.wait()
    fetch.wait()


def embed_kernel(plan, codes, table, resample, raising, placement, out):
    place = lax.axis_index("tp")
    core, pair = place % 2, place // 2
    row = lax.broadcasted_iota(jnp.int32, (plan.vocab, plan.lanes), 0)
    blank = jnp.zeros((1, SLOT - plan.ctx), jnp.int32)
    slots = []
    for image in range(plan.pairs):
        both = codes[2 * image : 2 * image + 2, :]
        slots += [jnp.where(core == 0, both[:1], both[1:]), blank]
    picked = (row == jnp.concatenate(slots, axis=1)).astype(F32)
    looked = dot(table[...], picked, precision=lax.Precision.HIGHEST)
    mapped = dot(looked, resample[...], precision=lax.Precision.HIGHEST).astype(BF16)
    fixed = jnp.concatenate(
        [placement[...].astype(F32)] * plan.pairs
        + [jnp.zeros((plan.lanes - plan.used, plan.width), F32)],
        axis=0,
    )
    full = (dot(mapped, raising[...], ((0,), (0,))) + fixed)[: plan.dense].astype(BF16)
    for at in range(plan.pairs):

        @pl.when(pair == at)
        def _(at=at):
            out[...] = full[:, at * plan.pair_cols : (at + 1) * plan.pair_cols]


def project(plan, tick, pieces, shifts, weights, held, qkv, wide, scale_at, offset_at, turning):
    pairs = plan.pairs
    mine, other, near, far = weights
    half = plan.ticks * plan.pairs
    place = lax.axis_index("tp")
    core, pair = place % 2, place // 2
    cols, pair_cols, lanes = plan.cols, plan.pair_cols, plan.lanes
    if tick == 0:
        turning[plan.used :, :] = jnp.zeros((lanes - plan.used, plan.width), F32)
    for k in range(pairs):
        at = pair ^ k
        if tick:
            piece = jnp.concatenate(
                [
                    pieces[k][...].astype(F32),
                    jnp.zeros((lanes - plan.dense, pair_cols), F32),
                ],
                axis=0,
            )
            wide[pl.ds(pl.multiple_of(at * pair_cols, 16), pair_cols), :] = piece.T
        else:
            piece = pieces[k][: plan.dense, :].astype(F32)
            chunks = [
                piece[j * plan.tokens : (j + 1) * plan.tokens, :pair_cols] for j in range(pairs)
            ]
            piece = jnp.concatenate(chunks, axis=1)
            for place_at in range(pairs):

                @pl.when(at == place_at)
                def _(place_at=place_at, piece=piece):
                    turning[place_at * plan.tokens : (place_at + 1) * plan.tokens, :] = piece

        for side in range(2):
            start = pl.multiple_of(
                at * pair_cols + (core if side == 0 else 1 - core) * cols, 16
            )
            own = pl.ds(pl.multiple_of(core * half, 8), half)
            scale_at[pl.ds(start, cols), :] = spread(shifts[side][k][0, own, :], tick, plan)
            offset_at[pl.ds(start, cols), :] = spread(shifts[side][k][1, own, :], tick, plan)
    if tick == 0:
        wide[...] = turning[...].T
    value = wide[...]
    average = jnp.sum(value, axis=0, keepdims=True) * (1.0 / plan.width)
    centred = value - average
    variance = jnp.sum(centred * centred, axis=0, keepdims=True) * (1.0 / plan.width)
    result = centred * lax.rsqrt(variance + 1e-06) * (1.0 + scale_at[...]) + offset_at[...]
    tokens = result.astype(BF16)
    start = pl.multiple_of(pair * pair_cols, 16)
    held[...] = wide[pl.ds(start, pair_cols), :].astype(BF16)
    if plan.rows > pair_cols + plan.halo:
        qkv[:, pair_cols + plan.halo :, :] = jnp.zeros(
            (3, plan.rows - pair_cols - plan.halo, lanes), BF16
        )
    for part in range(3):
        start = pl.multiple_of(core * cols, 16)
        qkv[part, pl.ds(start, cols), :] = dot(mine[part], tokens).astype(BF16)
        start = pl.multiple_of((1 - core) * cols, 16)
        qkv[part, pl.ds(start, cols), :] = dot(other[part], tokens).astype(BF16)
        edge = jnp.where(core == 1, near[part].astype(F32), far[part].astype(F32)).astype(BF16)
        qkv[part, pair_cols : pair_cols + plan.halo, :] = dot(edge, tokens).astype(BF16)


def attend(plan, tick, stores, qkv, sharp, attended, cached, mixed_at):
    pairs, pair_cols, dim, lanes = plan.pairs, plan.pair_cols, plan.head_dim, plan.lanes
    pair = lax.axis_index("tp") // 2
    for k in range(pairs):
        slot = pl.multiple_of((pair ^ k) * SLOT, SLOT)
        cached[0, pl.ds(slot, SLOT), :] = stores[k][2 * tick]
        cached[1, pl.ds(slot, SLOT), :] = stores[k][2 * tick + 1]
    head_at = first_head(pair, pair_cols, dim)
    begin = head_at * dim - pair * pair_cols
    row = lax.broadcasted_iota(jnp.int32, (lanes, lanes), 0)
    lane = lax.broadcasted_iota(jnp.int32, (lanes, lanes), 1)
    image = image_of(lane, plan)
    old_ok = (row // SLOT == image) & (row % SLOT < plan.ctx)
    new_ok = (image_of(row, plan) == image) & (row < plan.used)
    queries, keys, values, lifts, key_scales = [], [], [], [], []
    for head in range(plan.most):
        at = pl.ds(pl.multiple_of(begin + head * dim, 16), dim)
        query, key, value = qkv[0, at, :], qkv[1, at, :], qkv[2, at, :]
        wide_query, wide_key = query.astype(F32), key.astype(F32)
        lift = sharp[0, jnp.minimum(head_at + head, plan.heads - 1)]
        lift = jnp.exp(jnp.minimum(jnp.full((1, lanes), lift, F32), LOG_CAP))
        lifts.append(
            lax.rsqrt(jnp.sum(wide_query * wide_query, axis=0, keepdims=True) + 1e-06) * lift
        )
        key_scales.append(lax.rsqrt(jnp.sum(wide_key * wide_key, axis=0, keepdims=True) + 1e-06))
        queries.append(query)
        keys.append(key)
        values.append(value)
    pad = -plan.most % 8
    key_cols = jnp.concatenate(
        key_scales + ([jnp.zeros((pad, lanes), F32)] if pad else []), axis=0
    ).T
    old_keys, old_values = cached[0], cached[1]
    for head in range(plan.most):
        span = slice(head * dim, (head + 1) * dim)
        old = dot(old_keys[:, span], queries[head]) * lifts[head]
        new = (
            dot(keys[head], queries[head], ((0,), (0,)))
            * key_cols[:, head : head + 1]
            * lifts[head]
        )
        old = jnp.where(old_ok, old, -1e30)
        new = jnp.where(new_ok, new, -1e30)
        top = jnp.maximum(
            jnp.max(old, axis=0, keepdims=True), jnp.max(new, axis=0, keepdims=True)
        )
        old, new = jnp.exp(old - top), jnp.exp(new - top)
        total = 1.0 / (jnp.sum(old, axis=0, keepdims=True) + jnp.sum(new, axis=0, keepdims=True))
        old, new = (old * total).astype(BF16), (new * total).astype(BF16)
        mixed = dot(old_values[:, span], old, ((0,), (0,))) + dot(values[head], new)
        mixed_at[head * dim : (head + 1) * dim, :] = mixed
    attended[...] = mixed_at[...].T[: plan.dense].astype(BF16)


def project_kernel(plan, tick, *refs):
    pairs = plan.pairs
    project(
        plan,
        tick,
        refs[:pairs],
        (refs[pairs : 2 * pairs], refs[2 * pairs : 3 * pairs]),
        refs[3 * pairs : 3 * pairs + 4],
        *refs[3 * pairs + 4 :],
    )


def attend_kernel(plan, *refs):
    attend(plan, 0, refs[: plan.pairs], *refs[plan.pairs :])


def layer_kernel(plan, tick, *refs):
    pairs = plan.pairs
    attended, held, cached, mixed_at, qkv, *rest = refs[4 * pairs + 5 :]
    project(
        plan,
        tick,
        refs[:pairs],
        (refs[pairs : 2 * pairs], refs[2 * pairs : 3 * pairs]),
        refs[4 * pairs : 4 * pairs + 4],
        held,
        qkv,
        *rest,
    )
    attend(plan, tick, refs[3 * pairs : 4 * pairs], qkv, refs[4 * pairs + 4], attended, cached, mixed_at)


def return_kernel(plan, tick, *refs):
    pairs = plan.pairs
    pieces = refs[:pairs]
    mine, other, held, gate_mine, gate_other = refs[pairs : pairs + 5]
    rest = refs[pairs + 5 :]
    if tick == 0:
        entering, onward, *rows = rest[:-3]
    else:
        rows = rest[:-3]
    joined, projected, gate = rest[-3:]
    place = lax.axis_index("tp")
    core, pair = place % 2, place // 2
    cols, dim = plan.cols, plan.head_dim
    half = plan.ticks * pairs
    joined[plan.used :, :] = jnp.zeros((plan.lanes - plan.used, plan.width), BF16)
    for k in range(pairs):
        for at in range(pairs):

            @pl.when((pair ^ k) == at)
            def _(k=k, at=at):
                start, count = plan.starts[at] * dim, plan.counts[at] * dim
                joined[: plan.dense, start : start + count] = pieces[k][:, :count]

    value = joined[...]
    for side, (matrix, gates) in enumerate(((mine, gate_mine), (other, gate_other))):
        start = pl.multiple_of((core if side == 0 else 1 - core) * cols, 16)
        projected[pl.ds(start, cols), :] = dot(matrix[...], value, ((1,), (1,))).astype(BF16).astype(F32)
        gates = gates[pl.ds(pl.multiple_of(core * half, 8), half), :]
        gate[pl.ds(start, cols), :] = spread(gates, tick, plan)
    result = held[...].astype(F32) + gate[...] * projected[...]
    turned = result.T
    for k in range(pairs):
        for image in range(pairs):

            @pl.when((pair ^ k) == image)
            def _(k=k, image=image):
                rows[k][...] = turned[image * plan.tokens : (image + 1) * plan.tokens, :].astype(BF16)

    if tick == 0:
        last = lax.axis_index("section") == plan.section - 1
        onward[...] = jnp.where(last, entering[...].astype(F32), turned[: plan.dense]).astype(BF16)


def gather_kernel(plan, *refs):
    pairs = plan.pairs
    pieces, out, full = refs[:-2], refs[-2], refs[-1]
    pair = lax.axis_index("tp") // 2
    for tick in range(plan.ticks):
        for k in range(pairs):
            for at in range(pairs):

                @pl.when((pair ^ k) == at)
                def _(tick=tick, k=k, at=at):
                    full[tick, :, at * plan.pair_cols : (at + 1) * plan.pair_cols] = pieces[
                        tick * pairs + k
                    ][...].astype(F32)

    out[...] = jnp.stack([full[tick] for tick in range(plan.ticks)], axis=1).astype(BF16)


def resample_blocks(plan):
    blocks = []
    for coarse in range(1, SIDE):
        fine = np.arange(SIDE, dtype=np.float32)
        rough = np.arange(coarse, dtype=np.float32)
        one = np.float32(1.0)
        size, parts = np.float32(SIDE), np.float32(coarse)
        begins = np.maximum(fine[:, None] / size, rough[None, :] / parts)
        finish = np.minimum((fine[:, None] + one) / size, (rough[None, :] + one) / parts)
        crossing = np.maximum(finish - begins, np.float32(0.0)) * size
        blocks.append(
            (crossing[:, None, :, None] * crossing[None, :, None, :]).reshape(
                SIDE * SIDE, coarse * coarse
            )
        )
    table = np.concatenate(blocks, axis=1).astype(np.float32)
    full = np.zeros((plan.lanes, plan.lanes), np.float32)
    for image in range(plan.pairs):
        at = image * SLOT
        to = image * plan.tokens
        full[at : at + table.shape[1], to : to + table.shape[0]] = table.T
    return full


def paired(plan, *args):
    (
        awaiting_arrivals,
        label_numbers,
        drawn_coarse_codes,
        discrete_prototypes,
        code_raising_operator,
        placement_tier_features,
        label_feature_rows,
        conditioned_gain_mapping,
        conditioned_shift_addend,
        question_answer_operator,
        mixing_return_operator,
        focus_sharpness_exponents,
        prior_resolution_probes,
        prior_resolution_answers,
    ) = args
    pairs, tp, cols, pair_cols = plan.pairs, plan.tp, plan.cols, plan.pair_cols
    width, lanes, dim, ticks = plan.width, plan.lanes, plan.head_dim, plan.ticks
    rows = ticks * plan.images

    def swap(value, k):
        return lax.ppermute(value, "tp", [(g, g ^ (2 * k)) for g in range(tp)])

    def across(value):
        return lax.ppermute(value, "tp", [(g, g ^ 1) for g in range(tp)])

    def around(value):
        return [value] + [swap(value, k) for k in range(1, pairs)]

    def call(kernel, outs, scratch, values, scalars=(), loose=(), raw=(), space=pltpu.VMEM):
        ins = [
            pltpu.with_memory_space_constraint(
                v, pltpu.HBM if i in (*scalars, *loose, *raw) else pltpu.VMEM
            )
            for i, v in enumerate(values)
        ]
        return pl.pallas_call(
            lambda *refs: kernel(plan, *refs),
            out_shape=[space(shape, dtype) for shape, dtype in outs],
            in_specs=[
                pl.BlockSpec(
                    memory_space=pltpu.SMEM
                    if i in scalars
                    else pl.ANY
                    if i in raw
                    else pltpu.VMEM
                )
                for i in range(len(values))
            ],
            out_specs=[pl.BlockSpec(memory_space=pltpu.VMEM)] * len(outs),
            scratch_shapes=scratch,
            compiler_params=pltpu.CompilerParams(vmem_limit_bytes=KERNEL_VMEM),
        )(*ins)

    span = plan.most * dim
    qkv_mine = jnp.transpose(question_answer_operator[0], (1, 2, 0))
    active, edge, mod_matrix, first, *stores = call(
        opening_kernel,
        [
            ((rows, cols), BF16),
            ((3, plan.halo, width), BF16),
            ((3, cols, width), BF16),
            ((plan.dense, span), BF16),
        ]
        + [((2 * ticks, SLOT, span), BF16)] * pairs,
        [pltpu.VMEM((rows, plan.classes), F32), pltpu.SemaphoreType.DMA((2,))],
        [
            label_numbers,
            label_feature_rows.T,
            awaiting_arrivals[0, 0],
            jnp.transpose(prior_resolution_probes[0, :, 0], (1, 0, 2)),
            jnp.transpose(prior_resolution_answers[0, :, 0], (1, 0, 2)),
            qkv_mine,
            jnp.transpose(conditioned_gain_mapping[0], (1, 2, 0)),
        ],
        (0,),
        (1, 2, 3, 4),
        (5, 6),
    )
    active = around(active)
    active += [across(piece) for piece in active]
    shift, gate = call(
        modulation_kernel,
        [((2, rows, cols), F32), ((rows, cols), F32)],
        [pltpu.VMEM((width, 128), BF16)],
        [
            *active,
            mod_matrix,
            jnp.transpose(conditioned_shift_addend, (1, 0, 2)),
        ],
    )
    shifts = around(shift)
    shifts += [across(piece) for piece in shifts]
    gate_back = across(gate)

    qkv_other = across(qkv_mine)
    out_mine = mixing_return_operator[0].T
    out_other = across(out_mine)
    near = lax.ppermute(edge, "tp", [(2 * p + 2, 2 * p + 1) for p in range(pairs) if plan.need[p]])
    far = across(near)
    pieces = around(first)
    stored = [stores[0]] + [swap(stores[k], k) for k in range(1, pairs)]
    (entering,) = call(
        embed_kernel,
        [((plan.dense, pair_cols), BF16)],
        [],
        [
            drawn_coarse_codes[0],
            discrete_prototypes.T,
            jnp.asarray(resample_blocks(plan)),
            code_raising_operator,
            placement_tier_features,
        ],
    )

    emitted = []
    for tick in range(ticks):
        wide = [pltpu.VMEM((width, lanes), F32)] * 3 + [pltpu.VMEM((lanes, width), F32)]
        heads_of = [pltpu.VMEM((2, lanes, span), BF16), pltpu.VMEM((span, lanes), F32)]
        weights = [qkv_mine, qkv_other, near, far]
        if tick == 0:
            held, qkv = call(
                lambda *refs: project_kernel(refs[0], 0, *refs[1:]),
                [((pair_cols, lanes), BF16), ((3, plan.rows, lanes), BF16)],
                wide,
                [*pieces, *shifts, *weights],
            )
            (attended,) = call(
                attend_kernel,
                [((plan.dense, span), BF16)],
                heads_of,
                [*stored, qkv, focus_sharpness_exponents],
                (pairs + 1,),
            )
        else:
            values = [*pieces, *shifts, *stored, *weights, focus_sharpness_exponents]
            attended, held = call(
                lambda *refs, tick=tick: layer_kernel(refs[0], tick, *refs[1:]),
                [((plan.dense, span), BF16), ((pair_cols, lanes), BF16)],
                heads_of + [pltpu.VMEM((3, plan.rows, lanes), BF16)] + wide,
                values,
                (len(values) - 1,),
            )
        outs = [((plan.tokens, pair_cols), BF16)] * pairs
        extra = []
        if tick + 1 < ticks:
            outs = [((plan.dense, pair_cols), BF16)] + outs
            extra = [entering]
        results = call(
            lambda *refs, tick=tick: return_kernel(refs[0], tick, *refs[1:]),
            outs,
            [
                pltpu.VMEM((lanes, width), BF16),
                pltpu.VMEM((pair_cols, lanes), F32),
                pltpu.VMEM((pair_cols, lanes), F32),
            ],
            [
                *around(attended),
                out_mine,
                out_other,
                held,
                gate,
                gate_back,
                *extra,
            ],
        )
        if tick + 1 < ticks:
            onward = lax.ppermute(
                results[0],
                "section",
                [(s, (s + 1) % plan.section) for s in range(plan.section)],
            )
            pieces = around(onward)
        final = results[-pairs:]
        emitted += [final[0]] + [swap(final[k], k) for k in range(1, pairs)]
    (out,) = call(
        gather_kernel,
        [((plan.tokens, ticks, width), BF16)],
        [pltpu.VMEM((ticks, plan.tokens, width), F32)],
        emitted,
        space=pltpu.HBM,
    )
    return jnp.transpose(out, (1, 0, 2))[None, :, None]


def local(*args):
    plan = Plan(lax.axis_size("section"), lax.axis_size("tp"), args)
    return paired(plan, *args) if plan.fits else general(*args)


def solution(mesh):
    in_specs = (
        P("section", "tp", None, None),
        P(),
        P(),
        P(),
        P(),
        P(),
        P(None, "tp"),
        P("section", None, None, "tp"),
        P("section", None, "tp"),
        P("section", None, None, "tp"),
        P("section", None, "tp"),
        P("section", None),
        P("section", None, "tp", None, None),
        P("section", None, "tp", None, None),
    )
    out_specs = P("section", None, "tp", None, None)
    return jax.shard_map(local, mesh=mesh, in_specs=in_specs, out_specs=out_specs, check_vma=False)
```

```python
import jax
import jax.numpy as jnp
from jax import lax
from jax.experimental import pallas as pl
from jax.experimental.pallas import tpu as pltpu
from jax.sharding import PartitionSpec as P
import numpy as np

FOCUS_GROUPS = 30
HEAD_DIM = 64
SIDE = 5


LOG_CAP = 4.605170185988092


def shifted(value, axis, steps):
    count = lax.axis_size(axis)
    first, last = (max(0, -steps), min(count, count - steps))
    return lax.ppermute(value, axis, [(source, source + steps) for source in range(first, last)])


def crossing_matrix(target, coarse):
    fine_index = jnp.arange(target, dtype=jnp.float32)
    coarse_index = jnp.arange(coarse, dtype=jnp.float32)
    begins = jnp.maximum(fine_index[:, None] / target, coarse_index[None, :] / coarse)
    finish = jnp.minimum(
        (fine_index[:, None] + 1.0) / target, (coarse_index[None, :] + 1.0) / coarse
    )
    return jnp.maximum(finish - begins, 0.0) * target


def resampler():
    blocks = []
    for coarse in range(1, SIDE):
        crossing = crossing_matrix(SIDE, coarse)
        blocks.append(
            (crossing[:, None, :, None] * crossing[None, :, None, :]).reshape(
                SIDE * SIDE, coarse * coarse
            )
        )
    return jnp.concatenate(blocks, axis=1)


def embed(
    drawn_coarse_codes,
    discrete_prototypes,
    code_raising_operator,
    placement_tier_features,
    resample_table,
):
    looked_up = discrete_prototypes[drawn_coarse_codes]
    mapped = jnp.einsum(
        "tc,nicv->nitv", resample_table, looked_up, precision=lax.Precision.HIGHEST
    ).astype(jnp.bfloat16)
    leading = mapped.shape[:3]
    projected_rows = jnp.dot(
        mapped.reshape(-1, mapped.shape[3]),
        code_raising_operator,
        preferred_element_type=jnp.float32,
    )
    projected_rows = projected_rows.reshape(leading + (code_raising_operator.shape[1],))
    return (projected_rows + placement_tier_features.astype(jnp.float32)).astype(jnp.bfloat16)


def norm_mod(latent_stream, scale_term, offset_term):
    widened = latent_stream.astype(jnp.float32)
    average = jnp.mean(widened, axis=-1, keepdims=True)
    centred = widened - average
    spread = jnp.mean(centred * centred, axis=-1, keepdims=True)
    normed = (
        centred * lax.rsqrt(spread + 1e-06) * (1.0 + scale_term[:, None, :])
        + offset_term[:, None, :]
    )
    return normed.astype(jnp.bfloat16)


def attention(qkv_cols, log_scale, cached_keys, cached_values):
    qkv = lax.all_to_all(qkv_cols, "tp", split_axis=0, concat_axis=3, tiled=True)
    images = qkv.shape[0]
    count = qkv.shape[1]
    widened = qkv.astype(jnp.float32)
    query = widened[:, :, 0].reshape(images, count, FOCUS_GROUPS, HEAD_DIM)
    new_keys = widened[:, :, 1].reshape(images, count, FOCUS_GROUPS, HEAD_DIM)
    new_values = qkv[:, :, 2].reshape(images, count, FOCUS_GROUPS, HEAD_DIM)
    head_mult = jnp.exp(jnp.minimum(log_scale, LOG_CAP))
    query = (
        query
        * lax.rsqrt(jnp.sum(query * query, axis=-1, keepdims=True) + 1e-06)
        * head_mult[:, None]
    )
    new_keys = new_keys * lax.rsqrt(jnp.sum(new_keys * new_keys, axis=-1, keepdims=True) + 1e-06)
    all_keys = jnp.concatenate(
        [cached_keys.astype(jnp.float32).reshape(images, -1, FOCUS_GROUPS, HEAD_DIM), new_keys],
        axis=1,
    )
    all_values = jnp.concatenate(
        [cached_values.reshape(images, -1, FOCUS_GROUPS, HEAD_DIM), new_values], axis=1
    )
    scores = jnp.einsum("iqhd,ikhd->ihqk", query, all_keys, precision=lax.Precision.HIGHEST)
    maximum = jnp.max(scores, axis=-1, keepdims=True)
    weights = jnp.exp(scores - maximum)
    probabilities = (weights / jnp.sum(weights, axis=-1, keepdims=True)).astype(jnp.bfloat16)
    mixed = jnp.einsum(
        "ihqk,ikhd->iqhd", probabilities, all_values, preferred_element_type=jnp.float32
    )
    return mixed.reshape(images, count, FOCUS_GROUPS * HEAD_DIM).astype(jnp.bfloat16)


def project_out(attended, out_matrix):
    return jnp.dot(
        lax.all_gather(attended, "tp", axis=0, tiled=True),
        out_matrix,
        preferred_element_type=jnp.float32,
    )


def pass_on(latent_stream):
    return shifted(latent_stream, "section", 1)


def general(
    awaiting_arrivals,
    label_numbers,
    drawn_coarse_codes,
    discrete_prototypes,
    code_raising_operator,
    placement_tier_features,
    label_feature_rows,
    conditioned_gain_mapping,
    conditioned_shift_addend,
    question_answer_operator,
    mixing_return_operator,
    focus_sharpness_exponents,
    prior_resolution_probes,
    prior_resolution_answers,
):
    sections = lax.axis_size("section")
    section_at = lax.axis_index("section")
    group_index = lax.axis_index("tp")
    moments = prior_resolution_probes.shape[1]
    width = question_answer_operator.shape[1]
    column_width = question_answer_operator.shape[3]
    images = drawn_coarse_codes.shape[1]
    resident_pictures = awaiting_arrivals.shape[1]
    class_rows = lax.dynamic_slice_in_dim(label_numbers, sections - 1 - section_at, moments, 0)
    class_part = jnp.take(label_feature_rows, class_rows, axis=0)
    activated_part = jax.nn.silu(class_part.astype(jnp.float32)).astype(jnp.bfloat16)
    gated_response = lax.all_gather(activated_part, "tp", axis=2, tiled=True)
    flat_active = gated_response.reshape(moments * images, width)
    inner_block = 0
    local_mod = conditioned_gain_mapping[inner_block].reshape(width, 3 * column_width)
    modulated = jnp.dot(flat_active, local_mod, preferred_element_type=jnp.float32)
    mod_list = [
        modulated.reshape(moments, images, 3, column_width) + conditioned_shift_addend[inner_block]
    ]
    mod_cols = jnp.stack(mod_list)
    resample_table = resampler()
    emitted = []
    mod_rows = lax.all_to_all(mod_cols, "tp", split_axis=2, concat_axis=4, tiled=True)
    own_tokens = lax.dynamic_slice_in_dim(
        drawn_coarse_codes, group_index * resident_pictures, resident_pictures, 1
    )
    entering = embed(
        own_tokens,
        discrete_prototypes,
        code_raising_operator,
        placement_tier_features,
        resample_table,
    )
    passed_along_activation = awaiting_arrivals[0]
    for clock_tick in range(moments):
        latent_stream = passed_along_activation
        inner_block = 0
        modulation = mod_rows[inner_block, clock_tick]
        normed = norm_mod(latent_stream, modulation[:, 1], modulation[:, 2])
        local_qkv = question_answer_operator[inner_block].reshape(width, 3 * column_width)

        def body_product(portion, offset, local_qkv=local_qkv):
            return jnp.dot(portion, local_qkv, preferred_element_type=jnp.float32).astype(
                jnp.bfloat16
            )

        qkv_cols = body_product(lax.all_gather(normed, "tp", axis=0, tiled=True), jnp.int32(0))
        qkv_cols = qkv_cols.reshape(qkv_cols.shape[0], qkv_cols.shape[1], 3, column_width)
        attended = attention(
            qkv_cols,
            focus_sharpness_exponents[inner_block],
            prior_resolution_probes[inner_block, clock_tick],
            prior_resolution_answers[inner_block, clock_tick],
        )
        projected_cols = project_out(attended, mixing_return_operator[inner_block]).astype(
            jnp.bfloat16
        )
        projected = lax.all_to_all(projected_cols, "tp", split_axis=0, concat_axis=2, tiled=True)
        latent_stream = (
            latent_stream.astype(jnp.float32)
            + modulation[:, 0][:, None, :] * projected.astype(jnp.float32)
        ).astype(jnp.bfloat16)
        emitted.append(latent_stream)
        if clock_tick + 1 < moments:
            arrived = pass_on(latent_stream)
            passed_along_activation = jnp.where(section_at == 0, entering[clock_tick], arrived)
    result = jnp.stack(emitted)
    return result[None]


SLOT = 32
F32 = jnp.float32
BF16 = jnp.bfloat16
KERNEL_VMEM = 16 * 1024 * 1024


def first_head(pair, pair_width, head_dim):
    return (2 * pair * pair_width + head_dim) // (2 * head_dim)


class Plan:
    def __init__(self, section, tp, args):
        (arrivals, _, codes, prototypes, _, placement, labels, gain, _, _, _, sharp, probes, _) = args
        self.section, self.tp = section, tp
        self.pairs = tp // 2
        self.width = gain.shape[1]
        self.cols = gain.shape[3]
        self.pair_cols = 2 * self.cols
        self.heads = sharp.shape[1]
        self.head_dim = self.width // self.heads
        self.tokens = placement.shape[0]
        self.ctx = probes.shape[3]
        self.ticks = probes.shape[1]
        self.images = codes.shape[1]
        self.resident = arrivals.shape[1]
        self.used = self.pairs * self.tokens
        self.dense = self.used + -self.used % 8
        self.lanes = self.pairs * SLOT
        self.classes = labels.shape[0]
        self.vocab, self.code_dim = prototypes.shape
        starts = [first_head(p, self.pair_cols, self.head_dim) for p in range(self.pairs + 1)]
        self.starts = starts
        self.counts = [starts[p + 1] - starts[p] for p in range(self.pairs)]
        self.most = max(self.counts)
        self.left = [p * self.pair_cols - starts[p] * self.head_dim for p in range(self.pairs)]
        self.need = [
            max(0, starts[p + 1] * self.head_dim - (p + 1) * self.pair_cols)
            for p in range(self.pairs)
        ]
        self.halo = max(self.need)
        self.rows = max(self.pair_cols + self.halo, self.most * self.head_dim - min(self.left))
        self.fits = (
            tp % 2 == 0
            and self.pairs & (self.pairs - 1) == 0
            and gain.shape[0] == 1
            and codes.shape[0] == 1
            and self.ticks == 2
            and self.resident == 1
            and self.images == tp
            and self.cols % 16 == 0
            and self.head_dim == HEAD_DIM
            and starts[-1] == self.heads
            and max(self.left) <= 0
            and all(offset % 16 == 0 for offset in self.left)
            and 0 < self.halo <= self.cols
            and self.halo % 16 == 0
            and self.tokens <= SLOT
            and self.ctx <= SLOT
            and self.lanes == 128
        )


def dot(left, right, contract=((1,), (0,)), precision=None):
    return lax.dot_general(
        left, right, (contract, ((), ())), preferred_element_type=F32, precision=precision
    )


def image_of(token, plan):
    image = jnp.zeros(token.shape, jnp.int32)
    for at in range(1, plan.pairs + 1):
        image += (token >= at * plan.tokens).astype(jnp.int32)
    return image


def spread(rows, tick, plan):
    part = rows[tick * plan.pairs : (tick + 1) * plan.pairs, :]
    parts = []
    for _ in range(3):
        rounded = part.astype(BF16).astype(F32)
        parts.append(rounded)
        part = part - rounded
    count = 3 * plan.pairs
    stacked = jnp.concatenate(parts, axis=0).astype(BF16)
    row = lax.broadcasted_iota(jnp.int32, (count, plan.lanes), 0)
    lane = lax.broadcasted_iota(jnp.int32, (count, plan.lanes), 1)
    pick = (row % plan.pairs == image_of(lane, plan)).astype(F32).astype(BF16)
    return dot(stacked, pick, ((0,), (0,)))


def modulation_kernel(plan, *refs):
    pairs = plan.pairs
    near, far = refs[:pairs], refs[pairs : 2 * pairs]
    matrix, addend, shift, gate, active = refs[2 * pairs :]
    place = lax.axis_index("tp")
    core, pair = place % 2, place // 2
    rows = plan.ticks * plan.images
    for k in range(pairs):
        for side, piece in enumerate((near[k], far[k])):
            value = piece[...].astype(F32)
            value = jnp.concatenate([value, jnp.zeros((128 - rows, plan.cols), F32)], axis=0).T
            start = (pair ^ k) * plan.pair_cols + (core if side == 0 else 1 - core) * plan.cols
            active[pl.ds(pl.multiple_of(start, 16), plan.cols), :] = value.astype(BF16)
    tokens = active[...]
    for part in range(3):
        value = dot(matrix[part], tokens).T[:rows] + addend[part]
        if part:
            shift[part - 1] = value
        else:
            gate[...] = value


def opening_kernel(
    plan, labels, table, arrival, probes, answers, matrix, gain, active, edge, gained, *outs
):
    *outs, picked, arrived = outs
    halo = pltpu.make_async_copy(matrix.at[:, : plan.halo, :], edge, arrived.at[0])
    halo.start()
    fetch = pltpu.make_async_copy(gain, gained, arrived.at[1])
    fetch.start()
    pairs = plan.pairs
    pair = lax.axis_index("tp") // 2
    section_at = lax.axis_index("section")
    place = lax.broadcasted_iota(jnp.int32, (1, plan.classes), 1)
    row = 0
    for core in range(2):
        for tick in range(plan.ticks):
            for other in range(pairs):
                label = labels[tick - section_at + plan.section - 1, 2 * other + core]
                picked[row : row + 1, :] = (place == label).astype(F32)
                row += 1
    value = dot(picked[...].astype(BF16), table[...], ((1,), (1,)))
    active[...] = (value / (1.0 + jnp.exp(-value))).astype(BF16)

    span = plan.most * plan.head_dim
    first, stores = outs[0], outs[1:]
    wide = arrival[...].astype(F32)
    chunks = []
    for at in range(pairs):
        chunk = wide[:, at * plan.pair_cols : (at + 1) * plan.pair_cols]
        chunks.append(
            jnp.concatenate([chunk, jnp.zeros((plan.tokens, span - plan.pair_cols), F32)], axis=1)
        )
    first[...] = jnp.concatenate(
        chunks + [jnp.zeros((first.shape[0] - pairs * plan.tokens, span), F32)], axis=0
    ).astype(BF16)

    for source, stored in enumerate((probes, answers)):
        full = stored[...].astype(F32)
        for tick in range(plan.ticks):
            value = full[:, tick, :]
            for at in range(pairs):
                start = plan.starts[at] * plan.head_dim
                reach = min(span, plan.width - start)
                part = value[:, start : start + reach]
                if reach < span:
                    part = jnp.concatenate(
                        [part, jnp.zeros((plan.ctx, span - reach), F32)], axis=1
                    )
                part = jnp.concatenate(
                    [part, jnp.zeros((SLOT - plan.ctx, span), F32)], axis=0
                ).astype(BF16)
                for k in range(pairs):

                    @pl.when((pair ^ k) == at)
                    def _(k=k, part=part, tick=tick, source=source):
                        stores[k][2 * tick + source] = part

    halo.wait()
    fetch.wait()


def embed_kernel(plan, codes, table, resample, raising, placement, out):
    place = lax.axis_index("tp")
    core, pair = place % 2, place // 2
    row = lax.broadcasted_iota(jnp.int32, (plan.vocab, plan.lanes), 0)
    blank = jnp.zeros((1, SLOT - plan.ctx), jnp.int32)
    slots = []
    for image in range(plan.pairs):
        both = codes[2 * image : 2 * image + 2, :]
        slots += [jnp.where(core == 0, both[:1], both[1:]), blank]
    picked = (row == jnp.concatenate(slots, axis=1)).astype(F32)
    looked = dot(table[...], picked, precision=lax.Precision.HIGHEST)
    mapped = dot(looked, resample[...], precision=lax.Precision.HIGHEST).astype(BF16)
    fixed = jnp.concatenate(
        [placement[...].astype(F32)] * plan.pairs
        + [jnp.zeros((plan.lanes - plan.used, plan.width), F32)],
        axis=0,
    )
    full = (dot(mapped, raising[...], ((0,), (0,))) + fixed)[: plan.dense].astype(BF16)
    for at in range(plan.pairs):

        @pl.when(pair == at)
        def _(at=at):
            out[...] = full[:, at * plan.pair_cols : (at + 1) * plan.pair_cols]


def fill_shifts(plan, tick, shifts, scale_at, offset_at):
    place = lax.axis_index("tp")
    core, pair = place % 2, place // 2
    cols, half = plan.cols, plan.ticks * plan.pairs
    own = pl.ds(pl.multiple_of(core * half, 8), half)
    for k in range(plan.pairs):
        for side in range(2):
            start = pl.multiple_of(
                (pair ^ k) * plan.pair_cols + (core if side == 0 else 1 - core) * cols, 16
            )
            scale_at[pl.ds(start, cols), :] = spread(shifts[side][k][0, own, :], tick, plan)
            offset_at[pl.ds(start, cols), :] = spread(shifts[side][k][1, own, :], tick, plan)


def expand_kernel(plan, *refs):
    pairs = plan.pairs
    shifts = (refs[:pairs], refs[pairs : 2 * pairs])
    gate_mine, gate_other, scale_at, offset_at, *gates = refs[2 * pairs :]
    core = lax.axis_index("tp") % 2
    half = plan.ticks * pairs
    fill_shifts(plan, plan.ticks - 1, shifts, scale_at, offset_at)
    own = pl.ds(pl.multiple_of(core * half, 8), half)
    for tick in range(plan.ticks):
        for side, gate in enumerate((gate_mine, gate_other)):
            start = pl.multiple_of((core if side == 0 else 1 - core) * plan.cols, 16)
            gates[tick][pl.ds(start, plan.cols), :] = spread(gate[own, :], tick, plan)


def project(plan, tick, pieces, shifts, weights, held, qkv, wide, scale_at, offset_at, turning):
    pairs = plan.pairs
    mine, other, near, far = weights
    place = lax.axis_index("tp")
    core, pair = place % 2, place // 2
    cols, pair_cols, lanes = plan.cols, plan.pair_cols, plan.lanes
    if tick == 0:
        turning[plan.used :, :] = jnp.zeros((lanes - plan.used, plan.width), F32)
    for k in range(pairs):
        at = pair ^ k
        if tick:
            piece = jnp.concatenate(
                [
                    pieces[k][...].astype(F32),
                    jnp.zeros((lanes - plan.dense, pair_cols), F32),
                ],
                axis=0,
            )
            wide[pl.ds(pl.multiple_of(at * pair_cols, 16), pair_cols), :] = piece.T
        else:
            piece = pieces[k][: plan.dense, :].astype(F32)
            chunks = [
                piece[j * plan.tokens : (j + 1) * plan.tokens, :pair_cols] for j in range(pairs)
            ]
            piece = jnp.concatenate(chunks, axis=1)
            for place_at in range(pairs):

                @pl.when(at == place_at)
                def _(place_at=place_at, piece=piece):
                    turning[place_at * plan.tokens : (place_at + 1) * plan.tokens, :] = piece

    if tick == 0:
        wide[...] = turning[...].T
        fill_shifts(plan, tick, shifts, scale_at, offset_at)
    value = wide[...]
    average = jnp.sum(value, axis=0, keepdims=True) * (1.0 / plan.width)
    centred = value - average
    variance = jnp.sum(centred * centred, axis=0, keepdims=True) * (1.0 / plan.width)
    result = centred * lax.rsqrt(variance + 1e-06) * (1.0 + scale_at[...]) + offset_at[...]
    tokens = result.astype(BF16)
    start = pl.multiple_of(pair * pair_cols, 16)
    held[...] = wide[pl.ds(start, pair_cols), :].astype(BF16)
    if plan.rows > pair_cols + plan.halo:
        qkv[:, pair_cols + plan.halo :, :] = jnp.zeros(
            (3, plan.rows - pair_cols - plan.halo, lanes), BF16
        )
    for part in range(3):
        start = pl.multiple_of(core * cols, 16)
        qkv[part, pl.ds(start, cols), :] = dot(mine[part], tokens).astype(BF16)
        start = pl.multiple_of((1 - core) * cols, 16)
        qkv[part, pl.ds(start, cols), :] = dot(other[part], tokens).astype(BF16)
        edge = jnp.where(core == 1, near[part].astype(F32), far[part].astype(F32)).astype(BF16)
        qkv[part, pair_cols : pair_cols + plan.halo, :] = dot(edge, tokens).astype(BF16)


def attend(plan, tick, stores, qkv, sharp, attended, cached, mixed_at):
    pairs, pair_cols, dim, lanes = plan.pairs, plan.pair_cols, plan.head_dim, plan.lanes
    pair = lax.axis_index("tp") // 2
    for k in range(pairs):
        slot = pl.multiple_of((pair ^ k) * SLOT, SLOT)
        cached[0, pl.ds(slot, SLOT), :] = stores[k][2 * tick]
        cached[1, pl.ds(slot, SLOT), :] = stores[k][2 * tick + 1]
    head_at = first_head(pair, pair_cols, dim)
    begin = head_at * dim - pair * pair_cols
    row = lax.broadcasted_iota(jnp.int32, (lanes, lanes), 0)
    lane = lax.broadcasted_iota(jnp.int32, (lanes, lanes), 1)
    image = image_of(lane, plan)
    old_ok = (row // SLOT == image) & (row % SLOT < plan.ctx)
    new_ok = (image_of(row, plan) == image) & (row < plan.used)
    queries, keys, values, lifts, key_scales = [], [], [], [], []
    for head in range(plan.most):
        at = pl.ds(pl.multiple_of(begin + head * dim, 16), dim)
        query, key, value = qkv[0, at, :], qkv[1, at, :], qkv[2, at, :]
        wide_query, wide_key = query.astype(F32), key.astype(F32)
        lift = sharp[0, jnp.minimum(head_at + head, plan.heads - 1)]
        lift = jnp.exp(jnp.minimum(jnp.full((1, lanes), lift, F32), LOG_CAP))
        lifts.append(
            lax.rsqrt(jnp.sum(wide_query * wide_query, axis=0, keepdims=True) + 1e-06) * lift
        )
        key_scales.append(lax.rsqrt(jnp.sum(wide_key * wide_key, axis=0, keepdims=True) + 1e-06))
        queries.append(query)
        keys.append(key)
        values.append(value)
    pad = -plan.most % 8
    key_cols = jnp.concatenate(
        key_scales + ([jnp.zeros((pad, lanes), F32)] if pad else []), axis=0
    ).T
    old_keys, old_values = cached[0], cached[1]
    for head in range(plan.most):
        span = slice(head * dim, (head + 1) * dim)
        old = dot(old_keys[:, span], queries[head]) * lifts[head]
        new = (
            dot(keys[head], queries[head], ((0,), (0,)))
            * key_cols[:, head : head + 1]
            * lifts[head]
        )
        old = jnp.where(old_ok, old, -1e30)
        new = jnp.where(new_ok, new, -1e30)
        top = jnp.maximum(
            jnp.max(old, axis=0, keepdims=True), jnp.max(new, axis=0, keepdims=True)
        )
        old, new = jnp.exp(old - top), jnp.exp(new - top)
        total = 1.0 / (jnp.sum(old, axis=0, keepdims=True) + jnp.sum(new, axis=0, keepdims=True))
        old, new = (old * total).astype(BF16), (new * total).astype(BF16)
        mixed = dot(old_values[:, span], old, ((0,), (0,))) + dot(values[head], new)
        mixed_at[head * dim : (head + 1) * dim, :] = mixed
    attended[...] = mixed_at[...].T[: plan.dense].astype(BF16)


def project_kernel(plan, tick, *refs):
    pairs = plan.pairs
    project(
        plan,
        tick,
        refs[:pairs],
        (refs[pairs : 2 * pairs], refs[2 * pairs : 3 * pairs]),
        refs[3 * pairs : 3 * pairs + 4],
        *refs[3 * pairs + 4 :],
    )


def attend_kernel(plan, *refs):
    attend(plan, 0, refs[: plan.pairs], *refs[plan.pairs :])


def layer_kernel(plan, tick, *refs):
    pairs = plan.pairs
    pieces, (scale_at, offset_at) = refs[:pairs], refs[pairs : pairs + 2]
    stores = refs[pairs + 2 : 2 * pairs + 2]
    weights, refs = refs[2 * pairs + 2 : 2 * pairs + 6], refs[2 * pairs + 6 :]
    sharp, attended, held, cached, mixed_at, qkv, wide = refs
    project(plan, tick, pieces, None, weights, held, qkv, wide, scale_at, offset_at, None)
    attend(plan, tick, stores, qkv, sharp, attended, cached, mixed_at)


def return_kernel(plan, tick, *refs):
    pairs = plan.pairs
    pieces = refs[:pairs]
    mine, other, held, gate = refs[pairs : pairs + 4]
    rest = refs[pairs + 4 :]
    if tick == 0:
        entering, onward, *rows = rest[:-2]
    else:
        rows = rest[:-2]
    joined, projected = rest[-2:]
    place = lax.axis_index("tp")
    core, pair = place % 2, place // 2
    cols, dim = plan.cols, plan.head_dim
    joined[plan.used :, :] = jnp.zeros((plan.lanes - plan.used, plan.width), BF16)
    for k in range(pairs):
        for at in range(pairs):

            @pl.when((pair ^ k) == at)
            def _(k=k, at=at):
                start, count = plan.starts[at] * dim, plan.counts[at] * dim
                joined[: plan.dense, start : start + count] = pieces[k][:, :count]

    value = joined[...]
    for side, matrix in enumerate((mine, other)):
        start = pl.multiple_of((core if side == 0 else 1 - core) * cols, 16)
        projected[pl.ds(start, cols), :] = dot(matrix[...], value, ((1,), (1,))).astype(BF16).astype(F32)
    result = held[...].astype(F32) + gate[...] * projected[...]
    turned = result.T
    for k in range(pairs):
        for image in range(pairs):

            @pl.when((pair ^ k) == image)
            def _(k=k, image=image):
                rows[k][...] = turned[image * plan.tokens : (image + 1) * plan.tokens, :].astype(BF16)

    if tick == 0:
        last = lax.axis_index("section") == plan.section - 1
        onward[...] = jnp.where(last, entering[...].astype(F32), turned[: plan.dense]).astype(BF16)


def gather_kernel(plan, *refs):
    pairs = plan.pairs
    pieces, out, full = refs[:-2], refs[-2], refs[-1]
    pair = lax.axis_index("tp") // 2
    for tick in range(plan.ticks):
        for k in range(pairs):
            for at in range(pairs):

                @pl.when((pair ^ k) == at)
                def _(tick=tick, k=k, at=at):
                    full[tick, :, at * plan.pair_cols : (at + 1) * plan.pair_cols] = pieces[
                        tick * pairs + k
                    ][...].astype(F32)

    out[...] = jnp.stack([full[tick] for tick in range(plan.ticks)], axis=1).astype(BF16)


def resample_blocks(plan):
    blocks = []
    for coarse in range(1, SIDE):
        fine = np.arange(SIDE, dtype=np.float32)
        rough = np.arange(coarse, dtype=np.float32)
        one = np.float32(1.0)
        size, parts = np.float32(SIDE), np.float32(coarse)
        begins = np.maximum(fine[:, None] / size, rough[None, :] / parts)
        finish = np.minimum((fine[:, None] + one) / size, (rough[None, :] + one) / parts)
        crossing = np.maximum(finish - begins, np.float32(0.0)) * size
        blocks.append(
            (crossing[:, None, :, None] * crossing[None, :, None, :]).reshape(
                SIDE * SIDE, coarse * coarse
            )
        )
    table = np.concatenate(blocks, axis=1).astype(np.float32)
    full = np.zeros((plan.lanes, plan.lanes), np.float32)
    for image in range(plan.pairs):
        at = image * SLOT
        to = image * plan.tokens
        full[at : at + table.shape[1], to : to + table.shape[0]] = table.T
    return full


def paired(plan, *args):
    (
        awaiting_arrivals,
        label_numbers,
        drawn_coarse_codes,
        discrete_prototypes,
        code_raising_operator,
        placement_tier_features,
        label_feature_rows,
        conditioned_gain_mapping,
        conditioned_shift_addend,
        question_answer_operator,
        mixing_return_operator,
        focus_sharpness_exponents,
        prior_resolution_probes,
        prior_resolution_answers,
    ) = args
    pairs, tp, cols, pair_cols = plan.pairs, plan.tp, plan.cols, plan.pair_cols
    width, lanes, dim, ticks = plan.width, plan.lanes, plan.head_dim, plan.ticks
    rows = ticks * plan.images

    def swap(value, k):
        return lax.ppermute(value, "tp", [(g, g ^ (2 * k)) for g in range(tp)])

    def across(value):
        return lax.ppermute(value, "tp", [(g, g ^ 1) for g in range(tp)])

    def around(value):
        return [value] + [swap(value, k) for k in range(1, pairs)]

    def call(kernel, outs, scratch, values, scalars=(), loose=(), raw=(), space=pltpu.VMEM):
        ins = [
            pltpu.with_memory_space_constraint(
                v, pltpu.HBM if i in (*scalars, *loose, *raw) else pltpu.VMEM
            )
            for i, v in enumerate(values)
        ]
        return pl.pallas_call(
            lambda *refs: kernel(plan, *refs),
            out_shape=[space(shape, dtype) for shape, dtype in outs],
            in_specs=[
                pl.BlockSpec(
                    memory_space=pltpu.SMEM
                    if i in scalars
                    else pl.ANY
                    if i in raw
                    else pltpu.VMEM
                )
                for i in range(len(values))
            ],
            out_specs=[pl.BlockSpec(memory_space=pltpu.VMEM)] * len(outs),
            scratch_shapes=scratch,
            compiler_params=pltpu.CompilerParams(vmem_limit_bytes=KERNEL_VMEM),
        )(*ins)

    span = plan.most * dim
    qkv_mine = jnp.transpose(question_answer_operator[0], (1, 2, 0))
    active, edge, mod_matrix, first, *stores = call(
        opening_kernel,
        [
            ((rows, cols), BF16),
            ((3, plan.halo, width), BF16),
            ((3, cols, width), BF16),
            ((plan.dense, span), BF16),
        ]
        + [((2 * ticks, SLOT, span), BF16)] * pairs,
        [pltpu.VMEM((rows, plan.classes), F32), pltpu.SemaphoreType.DMA((2,))],
        [
            label_numbers,
            label_feature_rows.T,
            awaiting_arrivals[0, 0],
            jnp.transpose(prior_resolution_probes[0, :, 0], (1, 0, 2)),
            jnp.transpose(prior_resolution_answers[0, :, 0], (1, 0, 2)),
            qkv_mine,
            jnp.transpose(conditioned_gain_mapping[0], (1, 2, 0)),
        ],
        (0,),
        (1, 2, 3, 4),
        (5, 6),
    )
    active = around(active)
    active += [across(piece) for piece in active]
    shift, gate = call(
        modulation_kernel,
        [((2, rows, cols), F32), ((rows, cols), F32)],
        [pltpu.VMEM((width, 128), BF16)],
        [
            *active,
            mod_matrix,
            jnp.transpose(conditioned_shift_addend, (1, 0, 2)),
        ],
    )
    shifts = around(shift)
    shifts += [across(piece) for piece in shifts]
    gate_back = across(gate)

    qkv_other = across(qkv_mine)
    out_mine = mixing_return_operator[0].T
    out_other = across(out_mine)
    near = lax.ppermute(edge, "tp", [(2 * p + 2, 2 * p + 1) for p in range(pairs) if plan.need[p]])
    far = across(near)
    pieces = around(first)
    stored = [stores[0]] + [swap(stores[k], k) for k in range(1, pairs)]
    (entering,) = call(
        embed_kernel,
        [((plan.dense, pair_cols), BF16)],
        [],
        [
            drawn_coarse_codes[0],
            discrete_prototypes.T,
            jnp.asarray(resample_blocks(plan)),
            code_raising_operator,
            placement_tier_features,
        ],
    )

    *later_shift, gate_0, gate_1 = call(
        expand_kernel,
        [((width, lanes), F32)] * 2 + [((pair_cols, lanes), F32)] * 2,
        [],
        [*shifts, gate, gate_back],
    )
    gates = (gate_0, gate_1)
    emitted = []
    for tick in range(ticks):
        wide = [pltpu.VMEM((width, lanes), F32)] * 3 + [pltpu.VMEM((lanes, width), F32)]
        heads_of = [pltpu.VMEM((2, lanes, span), BF16), pltpu.VMEM((span, lanes), F32)]
        weights = [qkv_mine, qkv_other, near, far]
        if tick == 0:
            held, qkv = call(
                lambda *refs: project_kernel(refs[0], 0, *refs[1:]),
                [((pair_cols, lanes), BF16), ((3, plan.rows, lanes), BF16)],
                wide,
                [*pieces, *shifts, *weights],
            )
            (attended,) = call(
                attend_kernel,
                [((plan.dense, span), BF16)],
                heads_of,
                [*stored, qkv, focus_sharpness_exponents],
                (pairs + 1,),
            )
        else:
            values = [*pieces, *later_shift, *stored, *weights, focus_sharpness_exponents]
            attended, held = call(
                lambda *refs, tick=tick: layer_kernel(refs[0], tick, *refs[1:]),
                [((plan.dense, span), BF16), ((pair_cols, lanes), BF16)],
                heads_of + [pltpu.VMEM((3, plan.rows, lanes), BF16), wide[0]],
                values,
                (len(values) - 1,),
            )
        outs = [((plan.tokens, pair_cols), BF16)] * pairs
        extra = []
        if tick + 1 < ticks:
            outs = [((plan.dense, pair_cols), BF16)] + outs
            extra = [entering]
        results = call(
            lambda *refs, tick=tick: return_kernel(refs[0], tick, *refs[1:]),
            outs,
            [pltpu.VMEM((lanes, width), BF16), pltpu.VMEM((pair_cols, lanes), F32)],
            [
                *around(attended),
                out_mine,
                out_other,
                held,
                gates[tick],
                *extra,
            ],
        )
        if tick + 1 < ticks:
            onward = lax.ppermute(
                results[0],
                "section",
                [(s, (s + 1) % plan.section) for s in range(plan.section)],
            )
            pieces = around(onward)
        final = results[-pairs:]
        emitted += [final[0]] + [swap(final[k], k) for k in range(1, pairs)]
    (out,) = call(
        gather_kernel,
        [((plan.tokens, ticks, width), BF16)],
        [pltpu.VMEM((ticks, plan.tokens, width), F32)],
        emitted,
        space=pltpu.HBM,
    )
    return jnp.transpose(out, (1, 0, 2))[None, :, None]


def local(*args):
    plan = Plan(lax.axis_size("section"), lax.axis_size("tp"), args)
    return paired(plan, *args) if plan.fits else general(*args)


def solution(mesh):
    in_specs = (
        P("section", "tp", None, None),
        P(),
        P(),
        P(),
        P(),
        P(),
        P(None, "tp"),
        P("section", None, None, "tp"),
        P("section", None, "tp"),
        P("section", None, None, "tp"),
        P("section", None, "tp"),
        P("section", None),
        P("section", None, "tp", None, None),
        P("section", None, "tp", None, None),
    )
    out_specs = P("section", None, "tp", None, None)
    return jax.shard_map(local, mesh=mesh, in_specs=in_specs, out_specs=out_specs, check_vma=False)
```
